128 devices in a mesh: seq: 2 (over core), depth: 2 (over z_hi), vocab: 32 (over z_lo, y, x).
Axes of the slice: x: 4, y: 4, z: 4 (z_hi: 2, z_lo: 2; z = z_hi * 2 + z_lo), core: 2. Of those that a mesh axis runs over, the one named last changes fastest.
Arguments:
- hidden: bfloat16 [2, 512, 7168], P('depth', ('seq', 'vocab')), may hold values from -24 to 24
- embedding: bfloat16 [64640, 7168], P(('seq', 'vocab')), may hold values from -1 to 1
- targets: int32 [2, 512], P('depth', ('seq', 'vocab')), may hold values from 0 to 64639
- mask: int32 [2, 512], P('depth', ('seq', 'vocab')), may hold values 0 or 1
Outputs:
- nll: float32 [2, 512], P('depth', ('seq', 'vocab'))
- loss: float32 [], replicated
- grad_norm: float32 [], replicated
The draws below stay inside these ranges and needn't reach their ends.
All inputs are finite; a program needn't handle non-finite values. No bound on the sum of `mask` on one device may be relied on, other than what follows from the above.
Results may differ from the reference program's by a relative error of at most 0.0023.
Values may be sent and summed in bfloat16 or wider, within the bound.
A program may use at most 128 MiB of HBM per device.

```python
import math
import jax
import jax.numpy as jnp
from jax import lax

D = 7168
VOC_DEV = 1010
TOKENS = 512
VOCAB = 64640


def shared_tables(key):
    base = jax.random.fold_in(key, 7)
    keys = jax.random.split(base, 10)
    table = jnp.clip(jax.random.normal(keys[0], (VOCAB, D), jnp.float32) * (3.0 / math.sqrt(D)), -1.0, 1.0)
    noise = jax.random.normal(keys[1], (2, TOKENS, D), jnp.float32)
    states = jnp.stack([noise[0], 0.9 * noise[0] + 0.44 * noise[1]])
    channels = jax.random.randint(keys[7], (8,), 0, D)
    sizes = jax.random.uniform(keys[8], (8,), jnp.float32, 6.0, 14.0)
    signs = jnp.where(jax.random.bernoulli(keys[9], 0.5, (8,)), jnp.float32(1.0), jnp.float32(-1.0))
    columns = jnp.arange(D, dtype=jnp.int32)
    shared = jnp.sum(jnp.where(channels[:, None] == columns[None, :], (sizes * signs)[:, None], jnp.float32(0.0)), axis=0)
    states = states + shared[None, None, :]
    return (table, jnp.clip(states, -24.0, 24.0))


def draw_hidden(key, part):
    table, states = shared_tables(key)
    return states.astype(jnp.bfloat16)


def draw_embedding(key, part):
    table, states = shared_tables(key)
    return table.astype(jnp.bfloat16)


def draw_targets(key, part):
    keys = jax.random.split(jax.random.fold_in(key, 11), 5)
    common = jax.random.randint(keys[0], (64,), 0, VOCAB)
    first = jax.random.randint(keys[1], (TOKENS + 1,), 0, 64)
    second = jax.random.randint(keys[2], (TOKENS + 1,), 0, 64)
    frequent = common[jnp.minimum(first, second)]
    spread = jax.random.randint(keys[3], (TOKENS + 1,), 0, VOCAB)
    select = jax.random.randint(keys[4], (TOKENS + 1,), 0, 4)
    sequence = jnp.where(select == 0, spread, frequent).astype(jnp.int32)
    return jnp.stack([sequence[:TOKENS], sequence[1:]]).astype(jnp.int32)


def with_ends(entries, own_key, smallest, high):
    extent = entries.shape
    index_at = [jax.random.randint(jax.random.fold_in(own_key, axis), (), 0, extent[axis]) for axis in range(len(extent))]
    entries = entries.at[tuple(index_at)].set(smallest)
    longest = extent.index(max(extent))
    index_at[longest] = (index_at[longest] + 1) % extent[longest]
    return entries.at[tuple(index_at)].set(high)


def setup_inputs(seed: int = 0) -> dict:
    streams_of = jax.random.split(jax.random.key(seed), 5)
    hidden = draw_hidden(jax.random.fold_in(streams_of[4], 71), 0)
    embedding = draw_embedding(jax.random.fold_in(streams_of[4], 71), 0)
    targets = draw_targets(jax.random.fold_in(streams_of[4], 71), 0)
    mask = with_ends((jax.random.randint(streams_of[3], (2, TOKENS), 0, 4) < 3).astype(jnp.int32), jax.random.fold_in(streams_of[3], 1), 0, 1)
    return {"hidden": hidden, "embedding": embedding, "targets": targets, "mask": mask}


def reference(hidden, embedding, targets, mask):
    ids = jnp.arange(VOCAB, dtype=jnp.int32)
    head_weights = (1.0, 0.3)
    loss = jnp.zeros((), jnp.float32)
    nll_rows = []
    grads = []
    for head in range(2):
        states = hidden[head]
        logits = lax.dot_general(states, embedding, (((1,), (1,)), ((), ())), preferred_element_type=jnp.float32)
        peak = lax.optimization_barrier(jnp.max(logits, axis=1))
        total = lax.optimization_barrier(jnp.sum(jnp.exp(logits - peak[:, None]), axis=1))
        lse = peak + jnp.log(total)
        onehot = targets[head][:, None] == ids[None, :]
        chosen = lax.optimization_barrier(jnp.sum(jnp.where(onehot, logits, jnp.zeros((), jnp.float32)), axis=1))
        nll = lse - chosen
        live = mask[head].astype(jnp.float32)
        coef = head_weights[head] / jnp.maximum(jnp.sum(live), jnp.float32(1.0))
        loss = loss + coef * jnp.sum(live * nll)
        grad_logits = (coef * live[:, None] * (jnp.exp(logits - lse[:, None]) - onehot.astype(jnp.float32))).astype(jnp.bfloat16)
        nll_rows.append(nll)
        grads.append(grad_logits)

    def block_square(index):
        start = (index * VOC_DEV).astype(jnp.int32)
        summed = jnp.zeros((VOC_DEV, D), jnp.float32)
        for head in range(2):
            piece = lax.dynamic_slice_in_dim(grads[head], start, VOC_DEV, 1)
            part = jnp.dot(piece.T, hidden[head], preferred_element_type=jnp.float32).astype(jnp.bfloat16)
            part = lax.optimization_barrier(part)
            summed = summed + part.astype(jnp.float32)
        return jnp.sum(summed * summed)
    squares = lax.map(block_square, jnp.arange(VOCAB // VOC_DEV, dtype=jnp.int32))
    grad_norm = jnp.sqrt(jnp.sum(squares))
    return (jnp.stack(nll_rows), loss, grad_norm)
```

```python
import functools

import jax
import jax.numpy as jnp
from jax import lax
from jax.experimental import pallas as pl
from jax.experimental.pallas import tpu as pltpu
from jax.sharding import Mesh
from jax.sharding import PartitionSpec as P

MESH = pl.DeviceIdType.MESH
F32 = jnp.float32
BF16 = jnp.bfloat16

VOC = 1010
VPAD = 1024
D = 7168
T = 512
SLICES = 7
WIDTH = D // SLICES
SUBS = 4
SUBW = WIDTH // SUBS
STEPS = 4
NEUTRAL = -1e30
SHIFT = 13.862943611198906
CYCLE = (5, 3, 4, 2)


def kernel(
    hid_ref, emb_ref, tgt_ref, mask_ref, out_ref,
    h, emb, hp, l, b, x, xall, w, wp, ep, y, yx,
    ints1, ints2, st1, st2, fin1, fin2, live_buf, cols_buf,
    hid_sem, emb_sem, hs, hr, xs, xr, hps, hpr, es, er,
    is1, ir1, is2, ir2, ss1, sr1, ss2, sr2, fs1, fr1, fs2, fr2,
):
    ms, md, mz, my, mx = (lax.axis_index(a) for a in ("s", "d", "zl", "y", "x"))
    zz = md * 2 + mz
    qx1, qx0 = mx // 2, (mx + mx // 2) % 2
    qy1, qy0 = my // 2, (my + my // 2) % 2
    mine = (ms, mz, qy1, qy0, qx1, qx0)
    partner = {
        5: {"x": mx + 1 - 2 * (mx % 2)},
        4: {"x": 3 - mx},
        3: {"y": my + 1 - 2 * (my % 2)},
        2: {"y": 3 - my},
        1: {"zl": 1 - mz},
        0: {"s": 1 - ms},
    }
    item = ((((ms * 2 + mz) * 2 + qy1) * 2 + qy0) * 2 + qx1) * 2 + qx0
    col_id = ms * 4 + zz
    plane_id = my * 4 + mx

    def col_peer(k):
        s = (ms + k // 4) % 2
        z = (zz + k % 4) % 4
        return s * 4 + z, {"s": s, "d": z // 2, "zl": z % 2}

    def plane_peer(k):
        yy = (my + k // 4) % 4
        xx = (mx + k % 4) % 4
        return yy * 4 + xx, {"y": yy, "x": xx}

    own = pltpu.make_async_copy(hid_ref.at[0], h.at[mine], hid_sem)
    own.start()

    def emb_copy(c):
        cs = pl.ds(pl.multiple_of(c * WIDTH, WIDTH), WIDTH)
        return pltpu.make_async_copy(emb_ref.at[:, cs], emb.at[:, cs], emb_sem.at[c])

    barrier = pltpu.get_barrier_semaphore()
    for k in range(1, 8):
        pl.semaphore_signal(barrier, inc=1, device_id=col_peer(k)[1], device_id_type=MESH)
    for k in range(1, 16):
        pl.semaphore_signal(barrier, inc=1, device_id=plane_peer(k)[1], device_id_type=MESH)
    for c in range(SLICES):
        emb_copy(c).start()

    lane = lax.broadcasted_iota(jnp.int32, (8, T), 1)
    row8 = lax.broadcasted_iota(jnp.int32, (8, T), 0)
    ints = jnp.zeros((8, T), jnp.int32)
    for i in range(8):
        here = lane == item * 8 + i
        ints = jnp.where(here & (row8 == md), tgt_ref[0, i], ints)
        ints = jnp.where(here & (row8 == 2 + md), mask_ref[0, i], ints)
    ints1[col_id] = ints
    own.wait()
    pl.semaphore_wait(barrier, 22)

    def sends(buf, my_slot, peer, count, ssem, rsem):
        out = []
        for k in range(1, count):
            _, dev = peer(k)
            out.append(pltpu.make_async_remote_copy(
                src_ref=buf.at[my_slot], dst_ref=buf.at[my_slot],
                send_sem=ssem.at[k], recv_sem=rsem.at[my_slot],
                device_id=dev, device_id_type=MESH))
        return out

    def arrive(buf, peer, count, ssem, rsem):
        for k in range(1, count):
            slot, dev = peer(k)
            pltpu.make_async_remote_copy(
                src_ref=buf.at[slot], dst_ref=buf.at[slot],
                send_sem=ssem.at[k], recv_sem=rsem.at[slot],
                device_id=dev, device_id_type=MESH).wait_recv()

    def box(held, flip, cs):
        index = []
        for dim in range(6):
            if dim in held:
                index.append(slice(None))
            elif dim == flip:
                index.append(1 - mine[dim])
            else:
                index.append(mine[dim])
        return tuple(index) + (slice(None), cs)

    def step_copy(buf, held, dim, cs, ssem, rsem, incoming=False):
        where = buf.at[box(held, dim if incoming else None, cs)]
        return pltpu.make_async_remote_copy(
            src_ref=where, dst_ref=where, send_sem=ssem, recv_sem=rsem,
            device_id=partner[dim], device_id_type=MESH)

    def cube_copy(buf, slots, sub, step, start, width, ssem, rsem, incoming=False):
        dims = [CYCLE[(sub + k) % 4] for k in range(4)]
        held = (1, *dims[:step])
        cs = pl.ds(pl.multiple_of(start + sub * width, width), width)
        k = 1 + sub * STEPS + step
        return step_copy(buf, held, dims[step], cs, ssem.at[(*slots, k)], rsem.at[(*slots, k)], incoming)

    def z_copy(buf, slots, start, width, ssem, rsem, incoming=False):
        cs = pl.ds(pl.multiple_of(start, width), width)
        return step_copy(buf, (), 1, cs, ssem.at[(*slots, 0)], rsem.at[(*slots, 0)], incoming)

    def core_copy(buf, slots, start, width, ssem, rsem, incoming=False):
        cs = pl.ds(pl.multiple_of(start, width), width)
        return step_copy(buf, (1, 2, 3, 4, 5), 0, cs, ssem.at[(*slots, 17)], rsem.at[(*slots, 17)], incoming)

    for c in range(SLICES):
        z_copy(h, (c,), c * WIDTH, WIDTH, hs, hr).start()
    hp_copy = pltpu.make_async_remote_copy(
        src_ref=h.at[mine], dst_ref=hp, send_sem=hps, recv_sem=hpr,
        device_id={"d": 1 - md}, device_id_type=MESH)
    hp_copy.start()
    for copy in sends(ints1, col_id, col_peer, 8, is1, ir1):
        copy.start()

    l[...] = jnp.zeros_like(l)
    b[...] = jnp.zeros_like(b)
    x[...] = jnp.zeros_like(x)
    h2 = h.reshape(T, D)

    def nt(lhs, rhs):
        return lax.dot_general(lhs, rhs, (((1,), (1,)), ((), ())), preferred_element_type=F32)

    def body(i, carry):
        c4 = i - 4

        @pl.when((c4 >= 0) & (c4 < SLICES))
        def _():
            for sub in range(SUBS):
                cube_copy(h, (c4,), sub, 3, c4 * WIDTH, SUBW, hs, hr, True).wait_recv()
            core_copy(h, (c4,), c4 * WIDTH, WIDTH, hs, hr).start()

        for step in (3, 2, 1):
            c = i - step

            @pl.when((c >= 0) & (c < SLICES))
            def _(c=c, step=step):
                for sub in range(SUBS):
                    cube_copy(h, (c,), sub, step - 1, c * WIDTH, SUBW, hs, hr, True).wait_recv()
                    cube_copy(h, (c,), sub, step, c * WIDTH, SUBW, hs, hr).start()

        @pl.when(i < SLICES)
        def _():
            z_copy(h, (i,), i * WIDTH, WIDTH, hs, hr, True).wait_recv()
            for sub in range(SUBS):
                cube_copy(h, (i,), sub, 0, i * WIDTH, SUBW, hs, hr).start()

        @pl.when(i == 3)
        def _():
            hp_copy.wait_recv()
            arrive(ints1, col_peer, 8, is1, ir1)
            ints2[plane_id] = sum(ints1[k] for k in range(8))
            for copy in sends(ints2, plane_id, plane_peer, 16, is2, ir2):
                copy.start()

        c5 = i - 5

        @pl.when(c5 >= 0)
        def _():
            core_copy(h, (c5,), c5 * WIDTH, WIDTH, hs, hr, True).wait_recv()
            emb_copy(c5).wait()
            cs = pl.ds(pl.multiple_of(c5 * WIDTH, WIDTH), WIDTH)

            def half(n, carry):
                ts = pl.ds(pl.multiple_of(n * 256, 256), 256)
                hn = h2[ts, cs]
                l[0:VOC, ts] += nt(emb[:, cs], hn)
                b[:, ts] += nt(h2[:, cs], hn)
                x[:, ts] += nt(hp[:, cs], hn)
                return carry

            lax.fori_loop(0, 2, half, 0)

        return carry

    lax.fori_loop(0, SLICES + 5, body, 0)

    arrive(ints2, plane_peer, 16, is2, ir2)
    ints = sum(ints2[k] for k in range(16))
    first_id = (ms * 32 + mz * 16 + my * 4 + mx) * VOC
    local_t = ints[0:2] - first_id
    local_t = jnp.where(local_t < VOC, local_t, -1)
    own_t = jnp.where(md == 0, local_t[0:1], local_t[1:2])
    other_t = jnp.where(md == 0, local_t[1:2], local_t[0:1])
    live_buf[0:2] = ints[2:4].astype(F32)

    xall[mine] = x[...]
    z_copy(xall, (), 0, T, xs, xr).start()

    tail = l[VOC - 2 : VPAD]
    tail_row = lax.broadcasted_iota(jnp.int32, tail.shape, 0)
    l[VOC - 2 : VPAD] = jnp.where(tail_row < 2, tail, NEUTRAL)
    blk = 64
    groups = blk // 8
    rows = lax.broadcasted_iota(jnp.int32, (blk, T), 0)

    def peak_body(i, carry):
        peak, chosen = carry
        at = pl.multiple_of(i * blk, blk)
        part = l[pl.ds(at, blk)]
        hit = (rows + at) == own_t
        peak = jnp.maximum(peak, jnp.max(part.reshape(groups, 8, T), axis=0))
        chosen = chosen + jnp.sum(jnp.where(hit, part, 0.0).reshape(groups, 8, T), axis=0)
        return peak, chosen

    peak, chosen = lax.fori_loop(
        0, VPAD // blk, peak_body,
        (jnp.full((8, T), NEUTRAL, F32), jnp.zeros((8, T), F32)))
    origin = jnp.max(peak, axis=0, keepdims=True) - SHIFT
    chosen = jnp.sum(chosen, axis=0, keepdims=True)

    def exp_body(i, total):
        at = pl.multiple_of(i * blk, blk)
        e = jnp.exp(l[pl.ds(at, blk)] - origin)
        hit = (rows + at) == own_t
        w[pl.ds(at, blk), 0:T] = jnp.where(hit, 0.0, e).astype(BF16)
        w[pl.ds(at, blk), T : 2 * T] = jnp.where(hit, 1.0, 0.0).astype(BF16)
        return total + jnp.sum(e.reshape(groups, 8, T), axis=0)

    total = lax.fori_loop(0, VPAD // blk, exp_body, jnp.zeros((8, T), F32))
    total = jnp.sum(total, axis=0, keepdims=True)
    stats = jnp.where(row8 < 2, NEUTRAL, jnp.zeros((8, T), F32))
    stats = jnp.where(row8 == md, origin, stats)
    stats = jnp.where(row8 == 2 + md, total, stats)
    stats = jnp.where(row8 == 4 + md, chosen, stats)
    st1[col_id] = stats
    for copy in sends(st1, col_id, col_peer, 8, ss1, sr1):
        copy.start()

    z_copy(xall, (), 0, T, xs, xr, True).wait_recv()
    for sub in range(SUBS):
        cube_copy(xall, (), sub, 0, 0, T // SUBS, xs, xr).start()

    half_rows = VPAD // 2
    theirs = pl.ds(pl.multiple_of((1 - md) * half_rows, half_rows), half_rows)
    ours = pl.ds(pl.multiple_of(md * half_rows, half_rows), half_rows)
    e_copy = pltpu.make_async_remote_copy(
        src_ref=w.at[theirs, pl.ds(0, T)], dst_ref=ep, send_sem=es, recv_sem=er,
        device_id={"d": 1 - md}, device_id_type=MESH)
    e_copy.start()

    def merge(parts):
        top = parts[0][0:2]
        for p in parts[1:]:
            top = jnp.maximum(top, p[0:2])
        tot = jnp.zeros((2, T), F32)
        pick = jnp.zeros((2, T), F32)
        for p in parts:
            tot = tot + p[2:4] * jnp.exp(p[0:2] - top)
            pick = pick + p[4:6]
        return top, tot, pick

    arrive(st1, col_peer, 8, ss1, sr1)
    top, tot, pick = merge([st1[k] for k in range(8)])
    st2[plane_id, 0:2] = top
    st2[plane_id, 2:4] = tot
    st2[plane_id, 4:6] = pick
    st2[plane_id, 6:8] = jnp.zeros((2, T), F32)
    for copy in sends(st2, plane_id, plane_peer, 16, ss2, sr2):
        copy.start()

    for step in (1, 2, 3):
        for sub in range(SUBS):
            cube_copy(xall, (), sub, step - 1, 0, T // SUBS, xs, xr, True).wait_recv()
            cube_copy(xall, (), sub, step, 0, T // SUBS, xs, xr).start()

    gb = 256

    def gram_own(i, carry):
        at = pl.multiple_of(i * gb, gb)
        brow = pl.multiple_of((i % (T // gb)) * gb, gb)
        lhs = w[:, pl.ds(at, gb)]
        bb = b[pl.ds(brow, gb), :]
        for n in range(2):
            part = lax.dot_general(
                lhs, w[:, n * T : (n + 1) * T], (((0,), (0,)), ((), ())),
                preferred_element_type=F32)
            y[pl.ds(at, gb), n * T : (n + 1) * T] = part * bb
        return carry

    lax.fori_loop(0, 2 * T // gb, gram_own, 0)

    def other_hot(i, carry):
        at = pl.multiple_of(i * blk, blk)
        hit = (rows + (at + md * half_rows)) == other_t
        wp[pl.ds(at, blk), T : 2 * T] = jnp.where(hit, 1.0, 0.0).astype(BF16)
        return carry

    lax.fori_loop(0, half_rows // blk, other_hot, 0)

    for sub in range(SUBS):
        cube_copy(xall, (), sub, 3, 0, T // SUBS, xs, xr, True).wait_recv()
    core_copy(xall, (), 0, T, xs, xr).start()

    e_copy.wait_recv()
    wp[:, 0:T] = ep[...]
    core_copy(xall, (), 0, T, xs, xr, True).wait_recv()
    x2 = xall.reshape(T, T)

    def gram_cross(i, carry):
        at = pl.multiple_of(i * gb, gb)
        brow = pl.multiple_of((i % (T // gb)) * gb, gb)
        lhs = wp[:, pl.ds(at, gb)]
        bb = x2[pl.ds(brow, gb), :]
        for n in range(2):
            part = lax.dot_general(
                lhs, w[ours, n * T : (n + 1) * T], (((0,), (0,)), ((), ())),
                preferred_element_type=F32)
            yx[pl.ds(at, gb), n * T : (n + 1) * T] = part * bb
        return carry

    lax.fori_loop(0, 2 * T // gb, gram_cross, 0)

    arrive(st2, plane_peer, 16, ss2, sr2)
    top, tot, pick = merge([st2[k] for k in range(16)])
    lse = top + jnp.log(tot)
    nll = lse - pick
    live = live_buf[0:2]
    weight = jnp.where(lax.broadcasted_iota(jnp.int32, (2, 1), 0) == 0, 1.0, 0.3).astype(F32)
    coef = weight / jnp.maximum(jnp.sum(live, axis=1, keepdims=True), 1.0)
    loss = jnp.sum(coef * jnp.sum(live * nll, axis=1, keepdims=True), axis=0, keepdims=True)
    scale = coef * live
    g = scale * (jnp.exp(pick - lse) - 1.0)
    partner_slot = ms * 4 + (1 - md) * 2 + mz
    origin_p = jnp.where(md == 0, st1[partner_slot, 1:2], st1[partner_slot, 0:1])

    def pair(a):
        return (jnp.where(md == 0, a[0:1], a[1:2]), jnp.where(md == 0, a[1:2], a[0:1]))

    scale_o, scale_p = pair(scale)
    lse_o, lse_p = pair(lse)
    g_o, g_p = pair(g)
    s_o = scale_o * jnp.exp(origin - lse_o)
    s_p = scale_p * jnp.exp(origin_p - lse_p)
    vecs = jnp.where(row8 == 0, s_o, jnp.where(row8 == 1, g_o, jnp.where(row8 == 2, s_p, jnp.where(row8 == 3, g_p, 0.0))))
    cols_buf[...] = vecs.T

    qb = 64

    def quad(i, carry):
        acc_s, acc_g = carry
        at = pl.multiple_of(i * qb, qb)
        cols = cols_buf[pl.ds(at, qb), :]
        at2 = pl.multiple_of(T + at, qb)
        so, go, sp, gp = (cols[:, k : k + 1] for k in range(4))
        sp, gp = 2.0 * sp, 2.0 * gp
        left = (so * y[pl.ds(at, qb), 0:T] + go * y[pl.ds(at2, qb), 0:T]
                + sp * yx[pl.ds(at, qb), 0:T] + gp * yx[pl.ds(at2, qb), 0:T])
        right = (so * y[pl.ds(at, qb), T : 2 * T] + go * y[pl.ds(at2, qb), T : 2 * T]
                 + sp * yx[pl.ds(at, qb), T : 2 * T] + gp * yx[pl.ds(at2, qb), T : 2 * T])
        acc_s = acc_s + jnp.sum(left.reshape(qb // 8, 8, T), axis=0)
        acc_g = acc_g + jnp.sum(right.reshape(qb // 8, 8, T), axis=0)
        return acc_s, acc_g

    zero = jnp.zeros((8, T), F32)
    acc_s, acc_g = lax.fori_loop(0, T // qb, quad, (zero, zero))
    q = jnp.sum(jnp.sum(acc_s * s_o + acc_g * g_o, axis=0, keepdims=True), axis=1, keepdims=True)
    fin1[col_id] = jnp.broadcast_to(q, (8, 128))
    for copy in sends(fin1, col_id, col_peer, 8, fs1, fr1):
        copy.start()

    def drain(c, carry):
        z_copy(h, (c,), c * WIDTH, WIDTH, hs, hr).wait_send()
        for sub in range(SUBS):
            for step in range(STEPS):
                cube_copy(h, (c,), sub, step, c * WIDTH, SUBW, hs, hr).wait_send()
        core_copy(h, (c,), c * WIDTH, WIDTH, hs, hr).wait_send()
        return carry

    lax.fori_loop(0, SLICES, drain, 0)
    z_copy(xall, (), 0, T, xs, xr).wait_send()
    for sub in range(SUBS):
        for step in range(STEPS):
            cube_copy(xall, (), sub, step, 0, T // SUBS, xs, xr).wait_send()
    core_copy(xall, (), 0, T, xs, xr).wait_send()
    hp_copy.wait_send()
    e_copy.wait_send()
    for args in (
        (ints1, col_id, col_peer, 8, is1, ir1), (ints2, plane_id, plane_peer, 16, is2, ir2),
        (st1, col_id, col_peer, 8, ss1, sr1), (st2, plane_id, plane_peer, 16, ss2, sr2),
    ):
        for copy in sends(*args):
            copy.wait_send()

    arrive(fin1, col_peer, 8, fs1, fr1)
    fin2[plane_id] = sum(fin1[k] for k in range(8))
    last = sends(fin2, plane_id, plane_peer, 16, fs2, fr2)
    for copy in last:
        copy.start()
    arrive(fin2, plane_peer, 16, fs2, fr2)
    norm = jnp.sqrt(jnp.maximum(sum(fin2[k] for k in range(16)), 0.0))
    nll_own, _ = pair(nll)
    out = jnp.where(row8 == 0, nll_own, jnp.where(row8 == 1, loss, norm[0:1, 0:1]))
    out_ref[...] = out
    for copy in sends(fin1, col_id, col_peer, 8, fs1, fr1) + last:
        copy.wait_send()


def local(hidden, embedding, targets, mask):
    dma = pltpu.SemaphoreType.DMA
    out = pl.pallas_call(
        kernel,
        out_shape=jax.ShapeDtypeStruct((8, T), F32),
        in_specs=[
            pl.BlockSpec(memory_space=pl.ANY),
            pl.BlockSpec(memory_space=pl.ANY),
            pl.BlockSpec(memory_space=pltpu.SMEM),
            pl.BlockSpec(memory_space=pltpu.SMEM),
        ],
        out_specs=pl.BlockSpec(memory_space=pltpu.VMEM),
        scratch_shapes=[
            pltpu.VMEM((2, 2, 2, 2, 2, 2, 8, D), BF16),
            pltpu.VMEM((VOC, D), BF16),
            pltpu.VMEM((8, D), BF16),
            pltpu.VMEM((VPAD, T), F32),
            pltpu.VMEM((T, T), F32),
            pltpu.VMEM((8, T), F32),
            pltpu.VMEM((2, 2, 2, 2, 2, 2, 8, T), F32),
            pltpu.VMEM((VPAD, 2 * T), BF16),
            pltpu.VMEM((VPAD // 2, 2 * T), BF16),
            pltpu.VMEM((VPAD // 2, T), BF16),
            pltpu.VMEM((2 * T, 2 * T), F32),
            pltpu.VMEM((2 * T, 2 * T), F32),
            pltpu.VMEM((8, 8, T), jnp.int32),
            pltpu.VMEM((16, 8, T), jnp.int32),
            pltpu.VMEM((8, 8, T), F32),
            pltpu.VMEM((16, 8, T), F32),
            pltpu.VMEM((8, 8, 128), F32),
            pltpu.VMEM((16, 8, 128), F32),
            pltpu.VMEM((8, T), F32),
            pltpu.VMEM((T, 8), F32),
            dma,
            dma((SLICES,)),
            dma((SLICES, 18)),
            dma((SLICES, 18)),
            dma((18,)),
            dma((18,)),
            dma,
            dma,
            dma,
            dma,
            dma((8,)), dma((8,)), dma((16,)), dma((16,)),
            dma((8,)), dma((8,)), dma((16,)), dma((16,)),
            dma((8,)), dma((8,)), dma((16,)), dma((16,)),
        ],
        compiler_params=pltpu.CompilerParams(collective_id=0, has_side_effects=True),
        name="heads",
    )(hidden, embedding, targets, mask)
    ms, mz, my, mx = (lax.axis_index(a) for a in ("s", "zl", "y", "x"))
    item = ((ms * 2 + mz) * 4 + my // 2 * 2 + (my + my // 2) % 2) * 4 + mx // 2 * 2 + (mx + mx // 2) % 2
    nll = lax.dynamic_slice(out, (0, item * 8), (1, 8))
    return (nll, out[1, 0], out[2, 0])


def solution(mesh):
    torus = Mesh(mesh.devices.reshape(2, 2, 2, 4, 4), ("s", "d", "zl", "y", "x"))
    group = ("s", "zl", "y", "x")
    return jax.shard_map(
        local,
        mesh=torus,
        in_specs=(P("d", group, None), P(group, None), P("d", group), P("d", group)),
        out_specs=(P("d", group), P(), P()),
        check_vma=False,
    )
```

```python
import jax
import jax.numpy as jnp
from jax import lax
from jax.experimental import pallas as pl
from jax.experimental.pallas import tpu as pltpu
from jax.sharding import Mesh
from jax.sharding import PartitionSpec as P

MESH = pl.DeviceIdType.MESH
F32 = jnp.float32
BF16 = jnp.bfloat16

VOC = 1010
VPAD = 1024
D = 7168
T = 512
SLICES = 7
WIDTH = D // SLICES
SUBS = 4
SUBW = WIDTH // SUBS
STEPS = 4
LAG = 2
NEUTRAL = -1e30
SHIFT = 13.862943611198906
CYCLE = (5, 3, 4, 2)


def kernel(
    hid_ref, emb_ref, tgt_ref, mask_ref, nll_ref, loss_ref, norm_ref,
    hx, emb, l, b, xall, w, wp, ep, y, yx,
    ints1, ints2, st1, st2, fin1, fin2, live_buf, cols_buf,
    hid_sem, emb_sem, hs, hr, xs, xr, hps, hpr, es, er,
    is1, ir1, is2, ir2, ss1, sr1, ss2, sr2, fs1, fr1, fs2, fr2,
):
    ms, md, mz, my, mx = (lax.axis_index(a) for a in ("s", "d", "zl", "y", "x"))
    zz = md * 2 + mz
    qx1, qx0 = mx // 2, (mx + mx // 2) % 2
    qy1, qy0 = my // 2, (my + my // 2) % 2
    mine = (ms, mz, qy1, qy0, qx1, qx0)
    partner = {
        5: {"x": mx + 1 - 2 * (mx % 2)},
        4: {"x": 3 - mx},
        3: {"y": my + 1 - 2 * (my % 2)},
        2: {"y": 3 - my},
        1: {"zl": 1 - mz},
        0: {"s": 1 - ms},
    }
    item = ((((ms * 2 + mz) * 2 + qy1) * 2 + qy0) * 2 + qx1) * 2 + qx0
    col_id = ms * 4 + zz
    plane_id = my * 4 + mx
    h2 = hx.at[pl.ds(0, T)]
    h = h2.reshape(2, 2, 2, 2, 2, 2, 8, D)
    partner_rows = hx.at[pl.ds(T, 8)]
    x2 = xall.reshape(T, T)

    def col_peer(k):
        z = (zz + k % 4) % 4
        return {"s": (ms + k // 4) % 2, "d": z // 2, "zl": z % 2}

    def plane_peer(k):
        return {"y": (my + k // 4) % 4, "x": (mx + k % 4) % 4}

    def zx_peer(k):
        return {"zl": (mz + k // 4) % 2, "x": (mx + k % 4) % 4}

    def zy_peer(k):
        return {"zl": (mz + k // 4) % 2, "y": (my + k % 4) % 4}

    def wait_bytes(ref, sem):
        pltpu.make_async_copy(ref, ref, sem).wait()

    def send(src, dst, ssem, rsem, dev):
        pltpu.make_async_remote_copy(
            src_ref=src, dst_ref=dst, send_sem=ssem, recv_sem=rsem,
            device_id=dev, device_id_type=MESH).start()

    own = pltpu.make_async_copy(hid_ref.at[0], h.at[mine], hid_sem)
    own.start()

    def emb_copy(c):
        cs = pl.ds(pl.multiple_of(c * WIDTH, WIDTH), WIDTH)
        return pltpu.make_async_copy(emb_ref.at[:, cs], emb.at[:, cs], emb_sem.at[c])

    barrier = pltpu.get_barrier_semaphore()
    greeted = [col_peer(k) for k in range(1, 8)] + [plane_peer(k) for k in range(1, 16)]
    greeted += [zx_peer(k) for k in range(5, 8)] + [zy_peer(k) for k in range(5, 8)]
    for dev in greeted:
        pl.semaphore_signal(barrier, inc=1, device_id=dev, device_id_type=MESH)
    for c in range(SLICES):
        emb_copy(c).start()

    lane = lax.broadcasted_iota(jnp.int32, (8, T), 1)
    row8 = lax.broadcasted_iota(jnp.int32, (8, T), 0)
    ints = jnp.zeros((8, T), jnp.int32)
    for i in range(8):
        here = lane == item * 8 + i
        ints = jnp.where(here & (row8 == md), tgt_ref[0, i], ints)
        ints = jnp.where(here & (row8 == 2 + md), mask_ref[0, i], ints)
    ints1[col_id] = ints
    l[...] = jnp.zeros_like(l)
    b[...] = jnp.zeros_like(b)
    own.wait()
    pl.semaphore_wait(barrier, len(greeted))

    def share(buf, my_slot, peer, count, ssem, rsem):
        for k in range(1, count):
            send(buf.at[my_slot], buf.at[my_slot], ssem, rsem, peer(k))

    def box(held, cs):
        return tuple(slice(None) if dim in held else mine[dim] for dim in range(6)) + (slice(None), cs)

    def columns(start, width):
        return pl.ds(pl.multiple_of(start, width), width)

    def cube_send(c, step):
        for sub in range(SUBS):
            dims = [CYCLE[(sub + k) % 4] for k in range(4)]
            where = h.at[box((1, *dims[:step]), columns(c * WIDTH + sub * SUBW, SUBW))]
            send(where, where, hs, hr.at[c, 1 + step], partner[dims[step]])

    def cube_wait(c, step):
        wait_bytes(h2.at[pl.ds(0, 16 * 2**step), columns(c * WIDTH, WIDTH)], hr.at[c, 1 + step])

    for c in range(SLICES):
        where = h.at[(*mine, slice(None), columns(c * WIDTH, WIDTH))]
        send(where, where, hs, hr.at[c, 0], partner[1])
    send(h.at[mine], partner_rows, hps, hpr, {"d": 1 - md})
    share(ints1, col_id, col_peer, 8, is1, ir1)

    def nt(lhs, rhs):
        return lax.dot_general(lhs, rhs, (((1,), (1,)), ((), ())), preferred_element_type=F32)

    def body(i, carry):
        c4 = i - 4 * LAG

        @pl.when((c4 >= 0) & (c4 < SLICES))
        def _():
            cube_wait(c4, 3)
            where = h.at[box((1, 2, 3, 4, 5), columns(c4 * WIDTH, WIDTH))]
            send(where, where, hs, hr.at[c4, 5], partner[0])

        for step in (3, 2, 1):
            c = i - step * LAG

            @pl.when((c >= 0) & (c < SLICES))
            def _(c=c, step=step):
                cube_wait(c, step - 1)
                cube_send(c, step)

        @pl.when(i < SLICES)
        def _():
            wait_bytes(h2.at[pl.ds(0, 8), columns(i * WIDTH, WIDTH)], hr.at[i, 0])
            cube_send(i, 0)

        @pl.when(i == 4)
        def _():
            wait_bytes(partner_rows, hpr)
            wait_bytes(ints1.at[pl.ds(0, 7)], ir1)
            ints2[plane_id] = sum(ints1[k] for k in range(8))
            share(ints2, plane_id, plane_peer, 16, is2, ir2)

        c5 = i - 4 * LAG - 1

        @pl.when(c5 >= 0)
        def _():
            wait_bytes(h2.at[pl.ds(0, 256), columns(c5 * WIDTH, WIDTH)], hr.at[c5, 5])
            emb_copy(c5).wait()
            cs = columns(c5 * WIDTH, WIDTH)

            def half(n, carry):
                ts = pl.ds(pl.multiple_of(n * 256, 256), 256)
                hn = h2[ts, cs]
                l[0:VOC, ts] += nt(emb[:, cs], hn)
                b[:, ts] += nt(hx[:, cs], hn)
                return carry

            lax.fori_loop(0, 2, half, 0)

        return carry

    lax.fori_loop(0, SLICES + 4 * LAG + 1, body, 0)

    xall[mine] = b[T : T + 8]
    left, right = pl.ds(0, T // 2), pl.ds(T // 2, T // 2)
    for k in range(1, 8):
        for cs, sem, peer in ((left, 0, zx_peer), (right, 1, zy_peer)):
            where = xall.at[(*mine, slice(None), cs)]
            send(where, where, xs, xr.at[sem], peer(k))

    wait_bytes(ints2.at[pl.ds(0, 15)], ir2)
    ints = sum(ints2[k] for k in range(16))
    first_id = (ms * 32 + mz * 16 + my * 4 + mx) * VOC
    local_t = ints[0:2] - first_id
    local_t = jnp.where(local_t < VOC, local_t, -1)
    own_t = jnp.where(md == 0, local_t[0:1], local_t[1:2])
    other_t = jnp.where(md == 0, local_t[1:2], local_t[0:1])
    live_buf[0:2] = ints[2:4].astype(F32)

    tail = l[VOC - 2 : VPAD]
    tail_row = lax.broadcasted_iota(jnp.int32, tail.shape, 0)
    l[VOC - 2 : VPAD] = jnp.where(tail_row < 2, tail, NEUTRAL)
    blk = 64
    groups = blk // 8
    rows = lax.broadcasted_iota(jnp.int32, (blk, T), 0)

    def peak_body(i, carry):
        peak, chosen = carry
        at = pl.multiple_of(i * blk, blk)
        part = l[pl.ds(at, blk)]
        hit = (rows + at) == own_t
        peak = jnp.maximum(peak, jnp.max(part.reshape(groups, 8, T), axis=0))
        chosen = chosen + jnp.sum(jnp.where(hit, part, 0.0).reshape(groups, 8, T), axis=0)
        return peak, chosen

    peak, chosen = lax.fori_loop(
        0, VPAD // blk, peak_body,
        (jnp.full((8, T), NEUTRAL, F32), jnp.zeros((8, T), F32)))
    origin = jnp.max(peak, axis=0, keepdims=True) - SHIFT
    chosen = jnp.sum(chosen, axis=0, keepdims=True)

    def exp_body(i, total):
        at = pl.multiple_of(i * blk, blk)
        e = jnp.exp(l[pl.ds(at, blk)] - origin)
        hit = (rows + at) == own_t
        w[pl.ds(at, blk), 0:T] = jnp.where(hit, 0.0, e).astype(BF16)
        w[pl.ds(at, blk), T : 2 * T] = jnp.where(hit, 1.0, 0.0).astype(BF16)
        return total + jnp.sum(e.reshape(groups, 8, T), axis=0)

    total = lax.fori_loop(0, VPAD // blk, exp_body, jnp.zeros((8, T), F32))
    total = jnp.sum(total, axis=0, keepdims=True)
    stats = jnp.where(row8 < 2, NEUTRAL, jnp.zeros((8, T), F32))
    stats = jnp.where(row8 == md, origin, stats)
    stats = jnp.where(row8 == 2 + md, total, stats)
    stats = jnp.where(row8 == 4 + md, chosen, stats)
    st1[col_id] = stats
    share(st1, col_id, col_peer, 8, ss1, sr1)

    half_rows = VPAD // 2
    theirs = pl.ds(pl.multiple_of((1 - md) * half_rows, half_rows), half_rows)
    ours = pl.ds(pl.multiple_of(md * half_rows, half_rows), half_rows)
    send(w.at[theirs, pl.ds(0, T)], ep, es, er, {"d": 1 - md})

    gb = 256

    def gram_own(i, carry):
        at = pl.multiple_of(i * gb, gb)
        brow = pl.multiple_of((i % (T // gb)) * gb, gb)
        lhs = w[:, pl.ds(at, gb)]
        bb = b[pl.ds(brow, gb), :]
        for n in range(2):
            part = lax.dot_general(
                lhs, w[:, n * T : (n + 1) * T], (((0,), (0,)), ((), ())),
                preferred_element_type=F32)
            y[pl.ds(at, gb), n * T : (n + 1) * T] = part * bb
        return carry

    lax.fori_loop(0, 2 * T // gb, gram_own, 0)

    def merge(parts):
        top = parts[0][0:2]
        for p in parts[1:]:
            top = jnp.maximum(top, p[0:2])
        tot = jnp.zeros((2, T), F32)
        pick = jnp.zeros((2, T), F32)
        for p in parts:
            tot = tot + p[2:4] * jnp.exp(p[0:2] - top)
            pick = pick + p[4:6]
        return top, tot, pick

    wait_bytes(st1.at[pl.ds(0, 7)], sr1)
    top, tot, pick = merge([st1[k] for k in range(8)])
    st2[plane_id, 0:2] = top
    st2[plane_id, 2:4] = tot
    st2[plane_id, 4:6] = pick
    st2[plane_id, 6:8] = jnp.zeros((2, T), F32)
    share(st2, plane_id, plane_peer, 16, ss2, sr2)

    wait_bytes(x2.at[pl.ds(0, 56), left], xr.at[0])
    wait_bytes(x2.at[pl.ds(0, 56), right], xr.at[1])
    for k in range(1, 4):
        for cs, sem, held, peer in ((left, 2, (1, 4, 5), {"y": (my + k) % 4}), (right, 3, (1, 2, 3), {"x": (mx + k) % 4})):
            where = xall.at[box(held, cs)]
            send(where, where, xs, xr.at[sem], peer)

    def other_hot(i, carry):
        at = pl.multiple_of(i * blk, blk)
        hit = (rows + (at + md * half_rows)) == other_t
        wp[pl.ds(at, blk), T : 2 * T] = jnp.where(hit, 1.0, 0.0).astype(BF16)
        return carry

    lax.fori_loop(0, half_rows // blk, other_hot, 0)

    wait_bytes(x2.at[pl.ds(0, 192), left], xr.at[2])
    wait_bytes(x2.at[pl.ds(0, 192), right], xr.at[3])
    where = xall.at[ms]
    send(where, where, xs, xr.at[4], partner[0])

    wait_bytes(st2.at[pl.ds(0, 15)], sr2)
    top, tot, pick = merge([st2[k] for k in range(16)])
    lse = top + jnp.log(tot)
    nll = lse - pick
    live = live_buf[0:2]
    weight = jnp.where(lax.broadcasted_iota(jnp.int32, (2, 1), 0) == 0, 1.0, 0.3).astype(F32)
    coef = weight / jnp.maximum(jnp.sum(live, axis=1, keepdims=True), 1.0)
    loss = jnp.sum(coef * jnp.sum(live * nll, axis=1, keepdims=True), axis=0, keepdims=True)
    scale = coef * live
    g = (scale * (jnp.exp(pick - lse) - 1.0)).astype(BF16).astype(F32)
    partner_slot = ms * 4 + (1 - md) * 2 + mz
    origin_p = jnp.where(md == 0, st1[partner_slot, 1:2], st1[partner_slot, 0:1])

    def pair(a):
        return (jnp.where(md == 0, a[0:1], a[1:2]), jnp.where(md == 0, a[1:2], a[0:1]))

    scale_o, scale_p = pair(scale)
    lse_o, lse_p = pair(lse)
    g_o, g_p = pair(g)
    s_o = scale_o * jnp.exp(origin - lse_o)
    s_p = scale_p * jnp.exp(origin_p - lse_p)
    vecs = jnp.where(row8 == 0, s_o, jnp.where(row8 == 1, g_o, jnp.where(row8 == 2, s_p, jnp.where(row8 == 3, g_p, 0.0))))
    cols_buf[...] = vecs.T

    wait_bytes(ep, er)
    wp[:, 0:T] = ep[...]
    wait_bytes(xall.at[ms], xr.at[4])

    def gram_cross(i, carry):
        at = pl.multiple_of(i * gb, gb)
        brow = pl.multiple_of((i % (T // gb)) * gb, gb)
        lhs = wp[:, pl.ds(at, gb)]
        bb = x2[pl.ds(brow, gb), :]
        for n in range(2):
            part = lax.dot_general(
                lhs, w[ours, n * T : (n + 1) * T], (((0,), (0,)), ((), ())),
                preferred_element_type=F32)
            yx[pl.ds(at, gb), n * T : (n + 1) * T] = part * bb
        return carry

    lax.fori_loop(0, 2 * T // gb, gram_cross, 0)

    qb = 64

    def quad(i, carry):
        acc_s, acc_g = carry
        at = pl.multiple_of(i * qb, qb)
        cols = cols_buf[pl.ds(at, qb), :]
        at2 = pl.multiple_of(T + at, qb)
        so, go, sp, gp = (cols[:, k : k + 1] for k in range(4))
        sp, gp = 2.0 * sp, 2.0 * gp
        lhs = (so * y[pl.ds(at, qb), 0:T] + go * y[pl.ds(at2, qb), 0:T]
               + sp * yx[pl.ds(at, qb), 0:T] + gp * yx[pl.ds(at2, qb), 0:T])
        rhs = (so * y[pl.ds(at, qb), T : 2 * T] + go * y[pl.ds(at2, qb), T : 2 * T]
               + sp * yx[pl.ds(at, qb), T : 2 * T] + gp * yx[pl.ds(at2, qb), T : 2 * T])
        acc_s = acc_s + jnp.sum(lhs.reshape(qb // 8, 8, T), axis=0)
        acc_g = acc_g + jnp.sum(rhs.reshape(qb // 8, 8, T), axis=0)
        return acc_s, acc_g

    zero = jnp.zeros((8, T), F32)
    acc_s, acc_g = lax.fori_loop(0, T // qb, quad, (zero, zero))
    q = jnp.sum(jnp.sum(acc_s * s_o + acc_g * g_o, axis=0, keepdims=True), axis=1, keepdims=True)
    fin1[col_id] = jnp.broadcast_to(q, (8, 128))
    share(fin1, col_id, col_peer, 8, fs1, fr1)

    wait_bytes(h2.at[pl.ds(0, T - 8)], hs)
    wait_bytes(x2.at[pl.ds(0, T - 8)], xs)
    wait_bytes(partner_rows, hps)
    wait_bytes(ep, es)
    wait_bytes(ints1.at[pl.ds(0, 7)], is1)
    wait_bytes(ints2.at[pl.ds(0, 15)], is2)
    wait_bytes(st1.at[pl.ds(0, 7)], ss1)
    wait_bytes(st2.at[pl.ds(0, 15)], ss2)
    nll_own, _ = pair(nll)
    turned = pltpu.roll(jnp.broadcast_to(nll_own, (8, T)), (T - item * 8) % T, 1)
    nll_ref[...] = turned[0:1, 0:8]
    loss_ref[...] = loss

    wait_bytes(fin1.at[pl.ds(0, 7)], fr1)
    fin2[plane_id] = sum(fin1[k] for k in range(8))
    share(fin2, plane_id, plane_peer, 16, fs2, fr2)
    wait_bytes(fin1.at[pl.ds(0, 7)], fs1)
    wait_bytes(fin2.at[pl.ds(0, 15)], fr2)
    norm = jnp.sqrt(jnp.maximum(sum(fin2[k] for k in range(16)), 0.0))
    norm_ref[...] = norm[0:1, 0:1]
    wait_bytes(fin2.at[pl.ds(0, 15)], fs2)


def local(hidden, embedding, targets, mask):
    dma = pltpu.SemaphoreType.DMA
    vmem, smem = pl.BlockSpec(memory_space=pltpu.VMEM), pl.BlockSpec(memory_space=pltpu.SMEM)
    whole = pl.BlockSpec(memory_space=pl.ANY)
    nll, loss, norm = pl.pallas_call(
        kernel,
        out_shape=(
            jax.ShapeDtypeStruct((1, 8), F32),
            jax.ShapeDtypeStruct((1, 1), F32),
            jax.ShapeDtypeStruct((1, 1), F32),
        ),
        in_specs=[whole, whole, smem, smem],
        out_specs=(vmem, vmem, vmem),
        scratch_shapes=[
            pltpu.VMEM((T + 8, D), BF16),
            pltpu.VMEM((VOC, D), BF16),
            pltpu.VMEM((VPAD, T), F32),
            pltpu.VMEM((T + 8, T), F32),
            pltpu.VMEM((2, 2, 2, 2, 2, 2, 8, T), F32),
            pltpu.VMEM((VPAD, 2 * T), BF16),
            pltpu.VMEM((VPAD // 2, 2 * T), BF16),
            pltpu.VMEM((VPAD // 2, T), BF16),
            pltpu.VMEM((2 * T, 2 * T), F32),
            pltpu.VMEM((2 * T, 2 * T), F32),
            pltpu.VMEM((8, 8, T), jnp.int32),
            pltpu.VMEM((16, 8, T), jnp.int32),
            pltpu.VMEM((8, 8, T), F32),
            pltpu.VMEM((16, 8, T), F32),
            pltpu.VMEM((8, 8, 128), F32),
            pltpu.VMEM((16, 8, 128), F32),
            pltpu.VMEM((8, T), F32),
            pltpu.VMEM((T, 8), F32),
            dma,
            dma((SLICES,)),
            dma,
            dma((SLICES, 6)),
            dma,
            dma((5,)),
            dma, dma, dma, dma,
            dma, dma, dma, dma,
            dma, dma, dma, dma,
            dma, dma, dma, dma,
        ],
        compiler_params=pltpu.CompilerParams(collective_id=0, has_side_effects=True),
        name="heads",
    )(hidden, embedding, targets, mask)
    return (nll, loss[0, 0], norm[0, 0])


def solution(mesh):
    torus = Mesh(mesh.devices.reshape(2, 2, 2, 4, 4), ("s", "d", "zl", "y", "x"))
    group = ("s", "zl", "y", "x")
    return jax.shard_map(
        local,
        mesh=torus,
        in_specs=(P("d", group, None), P(group, None), P("d", group), P("d", group)),
        out_specs=(P("d", group), P(), P()),
        check_vma=False,
    )
```

```python
import jax
import jax.numpy as jnp
from jax import lax
from jax.experimental import pallas as pl
from jax.experimental.pallas import tpu as pltpu
from jax.sharding import Mesh
from jax.sharding import PartitionSpec as P

MESH = pl.DeviceIdType.MESH
F32 = jnp.float32
BF16 = jnp.bfloat16

VOC = 1010
VPAD = 1024
D = 7168
T = 512
SLICES = 7
WIDTH = D // SLICES
HALF = T // 2
SUBS = 4
SUBW = WIDTH // SUBS
LEAD = 2
LAG = 2
FIRST = SLICES + LEAD - 4 * LAG
TURN_A = SLICES + LEAD
NEUTRAL = -1e30
SHIFT = 13.862943611198906
CYCLE = (5, 3, 4, 2)


def kernel(
    hid_ref, emb_ref, tgt_ref, mask_ref, out_ref,
    hx, emb, l, b, xt, xall, w, wp, ep, y, yo, yx,
    ints1, ints2, st1, st2, fin1, fin2, live_buf, tgt_buf, orig_buf, tcols_buf, cols_buf,
    hid_sem, emb_sem, hs, hr, xs, xr, hps, hpr, es, er,
    is1, ir1, is2, ir2, ss1, sr1, ss2, sr2, fs1, fr1, fs2, fr2,
):
    ms, md, mz, my, mx = (lax.axis_index(a) for a in ("s", "d", "zl", "y", "x"))
    zz = md * 2 + mz
    qx1, qx0 = mx // 2, (mx + mx // 2) % 2
    qy1, qy0 = my // 2, (my + my // 2) % 2
    mine = (mz, ms, qy1, qy0, qx1, qx0)
    partner = {
        5: {"x": mx + 1 - 2 * (mx % 2)},
        4: {"x": 3 - mx},
        3: {"y": my + 1 - 2 * (my % 2)},
        2: {"y": 3 - my},
    }
    core, other_plane = {"s": 1 - ms}, {"zl": 1 - mz}
    item = ((((mz * 2 + ms) * 2 + qy1) * 2 + qy0) * 2 + qx1) * 2 + qx0
    col_id = ms * 4 + zz
    plane_id = my * 4 + mx
    h2 = hx.at[pl.ds(0, T)]
    h = h2.reshape(2, 2, 2, 2, 2, 2, 8, D)
    partner_rows = hx.at[pl.ds(T, 8)]
    x2 = xall.reshape(T, T)

    def col_peer(k):
        z = (zz + k % 4) % 4
        return {"s": (ms + k // 4) % 2, "d": z // 2, "zl": z % 2}

    def plane_peer(k):
        return {"y": (my + k // 4) % 4, "x": (mx + k % 4) % 4}

    def zx_peer(k):
        return {"zl": (mz + k // 4) % 2, "x": (mx + k % 4) % 4}

    def zy_peer(k):
        return {"zl": (mz + k // 4) % 2, "y": (my + k % 4) % 4}

    def wait_bytes(ref, sem):
        pltpu.make_async_copy(ref, ref, sem).wait()

    def send(src, dst, ssem, rsem, dev):
        pltpu.make_async_remote_copy(
            src_ref=src, dst_ref=dst, send_sem=ssem, recv_sem=rsem,
            device_id=dev, device_id_type=MESH).start()

    own = pltpu.make_async_copy(hid_ref.at[0], h.at[mine], hid_sem)
    own.start()

    def emb_copy(c):
        cs = pl.ds(pl.multiple_of(c * WIDTH, WIDTH), WIDTH)
        return pltpu.make_async_copy(emb_ref.at[:, cs], emb.at[:, cs], emb_sem.at[c])

    barrier = pltpu.get_barrier_semaphore()
    greeted = [col_peer(k) for k in range(1, 8)] + [plane_peer(k) for k in range(1, 16)]
    greeted += [zx_peer(k) for k in range(5, 8)] + [zy_peer(k) for k in range(5, 8)]
    for dev in greeted:
        pl.semaphore_signal(barrier, inc=1, device_id=dev, device_id_type=MESH)
    for c in range(SLICES):
        emb_copy(c).start()

    lane = lax.broadcasted_iota(jnp.int32, (8, T), 1)
    row8 = lax.broadcasted_iota(jnp.int32, (8, T), 0)
    ints = jnp.zeros((8, T), jnp.int32)
    for i in range(8):
        here = lane == item * 8 + i
        ints = jnp.where(here & (row8 == md), tgt_ref[0, i], ints)
        ints = jnp.where(here & (row8 == 2 + md), mask_ref[0, i], ints)
    ints1[col_id] = ints
    l[...] = jnp.zeros_like(l)
    b[...] = jnp.zeros_like(b)
    xt[...] = jnp.zeros_like(xt)
    own.wait()
    pl.semaphore_wait(barrier, len(greeted))

    def share(buf, my_slot, peer, count, ssem, rsem):
        for k in range(1, count):
            send(buf.at[my_slot], buf.at[my_slot], ssem, rsem, peer(k))

    def box(held, cs, plane=mz):
        at = (plane, *mine[1:])
        return tuple(slice(None) if dim in held else at[dim] for dim in range(6)) + (slice(None), cs)

    def columns(start, width):
        return pl.ds(pl.multiple_of(start, width), width)

    def slice_wait(unit, c, stage, items):
        wait_bytes(h2.at[pl.ds(0, 8 * items), columns(c * WIDTH, WIDTH)], hr.at[unit, stage])

    def x_peer(k):
        return {"x": (mx + k) % 4}

    def y_peer(k):
        return {"y": (my + k) % 4}

    def direct_send(c, stage):
        for sub, (first, second, held) in enumerate(((x_peer, y_peer, (4, 5)), (y_peer, x_peer, (2, 3)))):
            cs = columns(c * WIDTH + sub * (WIDTH // 2), WIDTH // 2)
            where = h.at[box(held if stage else (), cs)]
            for k in (2, 1, 3):
                send(where, where, hs, hr.at[c, stage], (second if stage else first)(k))

    def cube_send(c, step):
        for sub in range(SUBS):
            dims = [CYCLE[(sub + k) % 4] for k in range(4)]
            where = h.at[box(dims[:step], columns(c * WIDTH + sub * SUBW, SUBW), 1 - mz)]
            send(where, where, hs, hr.at[SLICES + c, 1 + step], partner[dims[step]])

    def core_send(unit, c, plane, stage):
        where = h.at[box((2, 3, 4, 5), columns(c * WIDTH, WIDTH), plane)]
        send(where, where, hs, hr.at[unit, stage], core)

    for c in range(SLICES):
        direct_send(c, 0)
    send(h.at[mine], partner_rows, hps, hpr, {"d": 1 - md})
    for c in range(SLICES):
        where = h.at[(*mine, slice(None), columns(c * WIDTH, WIDTH))]
        send(where, where, hs, hr.at[SLICES + c, 0], other_plane)
    share(ints1, col_id, col_peer, 8, is1, ir1)

    def nt(lhs, rhs):
        return lax.dot_general(lhs, rhs, (((1,), (1,)), ((), ())), preferred_element_type=F32)

    blk = 128
    groups = blk // 8
    rows = lax.broadcasted_iota(jnp.int32, (blk, HALF), 0)
    half_rows = VPAD // 2
    theirs = pl.ds(pl.multiple_of((1 - md) * half_rows, half_rows), half_rows)
    ours = pl.ds(pl.multiple_of(md * half_rows, half_rows), half_rows)

    def cross_columns(n):
        return tuple(columns(n * HALF + k * (HALF // 2), HALF // 2) for k in range(2))

    def cross_first(n, phase):
        xall[(*mine, slice(None), columns(n * HALF, HALF))] = xt[columns(n * HALF, HALF), :].T
        for k in range(1, 8):
            for sub, (cs, peer) in enumerate(zip(cross_columns(n), (zx_peer, zy_peer))):
                where = xall.at[(*mine, slice(None), cs)]
                send(where, where, xs, xr.at[phase, sub], peer(k))

    def cross_second(phase):
        for sub in range(2):
            wait_bytes(x2.at[pl.ds(0, 56), pl.ds(0, HALF // 2)], xr.at[phase, sub])
        for plane in range(2):
            halves = cross_columns(plane ^ phase)
            for k in (2, 1, 3):
                for sub, (cs, held, peer) in enumerate(zip(halves, ((4, 5), (2, 3)), (y_peer, x_peer))):
                    where = xall.at[box(held, cs, plane)]
                    send(where, where, xs, xr.at[phase, 2 + sub], peer(k))

    def cross_third(phase):
        for sub in range(2):
            wait_bytes(x2.at[pl.ds(0, 192), pl.ds(0, HALF // 2)], xr.at[phase, 2 + sub])
        for plane in range(2):
            where = xall.at[plane, ms, :, :, :, :, :, columns((plane ^ phase) * HALF, HALF)]
            send(where, where, xs, xr.at[phase, 4], core)

    def cross_wait(phase):
        wait_bytes(x2.at[pl.ds(0, 256), pl.ds(0, HALF)], xr.at[phase, 4])

    def finish_half(n, phase):
        ls = columns(n * HALF, HALF)
        cross_first(n, phase)
        own_t = tgt_buf[0:1, ls]

        def peak_body(i, carry):
            peak, chosen = carry
            at = pl.multiple_of(i * blk, blk)
            part = l[pl.ds(at, blk), ls]
            hit = (rows + at) == own_t
            peak = jnp.maximum(peak, jnp.max(part.reshape(groups, 8, HALF), axis=0))
            chosen = chosen + jnp.sum(jnp.where(hit, part, 0.0).reshape(groups, 8, HALF), axis=0)
            return peak, chosen

        peak, chosen = lax.fori_loop(
            0, VPAD // blk, peak_body,
            (jnp.full((8, HALF), NEUTRAL, F32), jnp.zeros((8, HALF), F32)))
        origin = jnp.max(peak, axis=0, keepdims=True) - SHIFT
        chosen = jnp.sum(chosen, axis=0, keepdims=True)

        def exp_body(i, total):
            at = pl.multiple_of(i * blk, blk)
            e = jnp.exp(l[pl.ds(at, blk), ls] - origin)
            hit = (rows + at) == own_t
            w[pl.ds(at, blk), ls] = jnp.where(hit, 0.0, e).astype(BF16)
            w[pl.ds(at, blk), columns(T + n * HALF, HALF)] = jnp.where(hit, 1.0, 0.0).astype(BF16)
            return total + jnp.sum(e.reshape(groups, 8, HALF), axis=0)

        total = lax.fori_loop(0, VPAD // blk, exp_body, jnp.zeros((8, HALF), F32))
        total = jnp.sum(total, axis=0, keepdims=True)
        st1[phase, plane_id] = tile(origin, total, chosen)
        orig_buf[0:1, ls] = origin
        share(st1.at[phase], plane_id, plane_peer, 16, ss1, sr1.at[phase])

    def tile(*lines):
        out = jnp.zeros((8, 128), F32)
        for k, line in enumerate(lines):
            for part in range(2):
                out = jnp.where(row8[:, 0:128] == 2 * k + part, line[:, part * 128 : (part + 1) * 128], out)
        return out

    def merge(parts):
        top = parts[0][0:2]
        for p in parts[1:]:
            top = jnp.maximum(top, p[0:2])
        tot = jnp.zeros((2, 128), F32)
        pick = jnp.zeros((2, 128), F32)
        for p in parts:
            tot = tot + p[2:4] * jnp.exp(p[0:2] - top)
            pick = pick + p[4:6]
        return top, tot, pick

    def plane_merge(n, phase):
        wait_bytes(st1.at[phase, pl.ds(0, 15)], sr1.at[phase])
        top, tot, pick = merge([st1[phase, k] for k in range(16)])
        st2[col_id, n, 0:2] = top
        st2[col_id, n, 2:4] = tot
        st2[col_id, n, 4:6] = pick
        own_origin = orig_buf[0:1, columns(n * HALF, HALF)]
        st2[col_id, n, 6:7] = own_origin[:, 0:128]
        st2[col_id, n, 7:8] = own_origin[:, 128:256]

    def exchange(n, phase):
        ls = columns(n * HALF, HALF)
        send(w.at[theirs, ls], ep.at[:, ls], es, er.at[phase], {"d": 1 - md})

    def body(i, carry):
        @pl.when(i < SLICES)
        def _():
            slice_wait(i, i, 0, 3)
            direct_send(i, 1)

        c = i - LEAD

        @pl.when((c >= 0) & (c < SLICES))
        def _():
            slice_wait(c, c, 1, 12)
            core_send(c, c, mz, 2)

        c4 = i - FIRST - 4 * LAG

        @pl.when((c4 >= 0) & (c4 < SLICES))
        def _():
            slice_wait(SLICES + c4, c4, 4, 8)
            core_send(SLICES + c4, c4, 1 - mz, 5)

        for step in (3, 2, 1, 0):
            c = i - FIRST - step * LAG

            @pl.when((c >= 0) & (c < SLICES))
            def _(c=c, step=step):
                slice_wait(SLICES + c, c, step, 2 ** max(step - 1, 0))
                cube_send(c, step)

        @pl.when(i == 5)
        def _():
            wait_bytes(ints1.at[pl.ds(0, 7)], ir1)
            ints2[plane_id] = sum(ints1[k] for k in range(8))
            share(ints2, plane_id, plane_peer, 16, is2, ir2)

        u = i - LEAD - 1

        @pl.when(u == 0)
        def _():
            wait_bytes(partner_rows, hpr)

        @pl.when(u >= 0)
        def _():
            phase = u // SLICES
            c = u - phase * SLICES
            n = mz + phase * (1 - 2 * mz)

            @pl.when(phase == 0)
            def _():
                slice_wait(c, c, 2, 16)
                emb_copy(c).wait()

            @pl.when(phase == 1)
            def _():
                slice_wait(SLICES + c, c, 5, 16)

            cs, ls = columns(c * WIDTH, WIDTH), columns(n * HALF, HALF)
            hn = h2[ls, cs]
            l[0:VOC, ls] += nt(emb[:, cs], hn)
            xt[ls, :] += nt(hn, partner_rows[:, cs])

            @pl.when(phase == 0)
            def _():
                b[ls, ls] += nt(hn, hn)


        @pl.when(i == TURN_A)
        def _():
            wait_bytes(ints2.at[pl.ds(0, 15)], ir2)
            ints = sum(ints2[k] for k in range(16))
            first_id = (ms * 32 + mz * 16 + my * 4 + mx) * VOC
            local_t = ints[0:2] - first_id
            local_t = jnp.where(local_t < VOC, local_t, -1)
            tgt_buf[0:1] = jnp.where(md == 0, local_t[0:1], local_t[1:2])
            tgt_buf[1:2] = jnp.where(md == 0, local_t[1:2], local_t[0:1])
            live_buf[0:2] = ints[2:4].astype(F32)
            tail = l[VOC - 2 : VPAD]
            tail_row = lax.broadcasted_iota(jnp.int32, tail.shape, 0)
            l[VOC - 2 : VPAD] = jnp.where(tail_row < 2, tail, NEUTRAL)
            finish_half(mz, 0)
            exchange(mz, 0)

        @pl.when(i == TURN_A + 3)
        def _():
            cross_second(0)

        @pl.when(i == TURN_A + 5)
        def _():
            plane_merge(mz, 0)

        @pl.when(i == TURN_A + 6)
        def _():
            cross_third(0)

        return carry

    lax.fori_loop(0, 2 * SLICES + LEAD + 1, body, 0)

    finish_half(1 - mz, 1)
    exchange(1 - mz, 1)

    own_cols, late_cols = columns(mz * HALF, HALF), columns((1 - mz) * HALF, HALF)

    def late_b(c, carry):
        cs = columns(c * WIDTH, WIDTH)
        b[:, late_cols] += nt(h2[:, cs], h2[late_cols, cs])
        return carry

    lax.fori_loop(0, SLICES, late_b, 0)
    cross_second(1)
    b[late_cols, own_cols] = b[own_cols, late_cols].T

    tgt_rows = jnp.where(row8 < 2, jnp.broadcast_to(tgt_buf[0:1], (8, T)), 0).astype(F32)
    tcols_buf[...] = tgt_rows.T

    def tn(lhs, rhs):
        return lax.dot_general(lhs, rhs, (((0,), (0,)), ((), ())), preferred_element_type=F32)

    def gram_own(i, carry):
        rs = columns(i * HALF, HALF)
        lhs = w[:, rs]
        bb = b[rs, :]
        y[rs, 0:T] = tn(lhs, w[:, 0:T]) * bb
        y[rs, T : 2 * T] = tn(lhs, w[:, T : 2 * T]) * (2.0 * bb)
        return carry

    lax.fori_loop(0, 2, gram_own, 0)

    other_t = tgt_buf[1:2]
    rows_full = lax.broadcasted_iota(jnp.int32, (blk, T), 0)

    def other_hot(i, carry):
        at = pl.multiple_of(i * blk, blk)
        hit = (rows_full + (at + md * half_rows)) == other_t
        wp[pl.ds(at, blk), :] = jnp.where(hit, 1.0, 0.0).astype(BF16)
        return carry

    lax.fori_loop(0, half_rows // blk, other_hot, 0)

    def same_target(i, carry):
        rs = pl.ds(pl.multiple_of(i * 64, 64), 64)
        own_row = tgt_buf[0:1].astype(F32)
        same = (tcols_buf[rs, 0:1] == own_row) & (own_row >= 0.0)
        yo[rs, :] = jnp.where(same, b[rs, :], 0.0)
        return carry

    lax.fori_loop(0, T // 64, same_target, 0)

    plane_merge(1 - mz, 1)
    share(st2, col_id, col_peer, 8, ss2, sr2)

    def gram_hot(i, carry):
        rs = columns(i * HALF, HALF)
        lhs = wp[:, rs]
        for n in range(2):
            yx[columns(T + i * HALF, HALF), n * T : (n + 1) * T] = tn(lhs, w[ours, n * T : (n + 1) * T])
        return carry

    lax.fori_loop(0, 2, gram_hot, 0)

    cross_third(1)

    for phase in range(2):
        wait_bytes(ep.at[:, pl.ds(0, HALF)], er.at[phase])

    def gram_cross(i, carry):
        rs = columns(i * HALF, HALF)
        lhs = ep[:, rs]
        for n in range(2):
            yx[rs, n * T : (n + 1) * T] = tn(lhs, w[ours, n * T : (n + 1) * T])
        return carry

    lax.fori_loop(0, 2, gram_cross, 0)

    wait_bytes(st2.at[pl.ds(0, 7)], sr2)
    def line(piece):
        return jnp.concatenate([piece(n)[k : k + 1] for n in range(2) for k in range(2)], axis=1)

    def both(first, second):
        return jnp.where(lax.broadcasted_iota(jnp.int32, (2, T), 0) == 0, first, second)

    merged = [[merge([st2[s * 4 + head * 2 + z, n] for s in range(2) for z in range(2)]) for n in range(2)] for head in range(2)]
    top, tot, pick = (both(*(line(lambda n: merged[head][n][k]) for head in range(2))) for k in range(3))
    lse = top + jnp.log(tot)
    nll = lse - pick
    live = live_buf[0:2]
    weight = jnp.where(lax.broadcasted_iota(jnp.int32, (2, 1), 0) == 0, 1.0, 0.3).astype(F32)
    coef = weight / jnp.maximum(jnp.sum(live, axis=1, keepdims=True), 1.0)
    loss = jnp.sum(coef * jnp.sum(live * nll, axis=1, keepdims=True), axis=0, keepdims=True)
    scale = coef * live
    g = (scale * (jnp.exp(pick - lse) - 1.0)).astype(BF16).astype(F32)
    partner_slot = ms * 4 + (1 - md) * 2 + mz
    origin_p = line(lambda n: st2[partner_slot, n, 6:8])
    origin = orig_buf[0:1]

    def pair(a):
        return (jnp.where(md == 0, a[0:1], a[1:2]), jnp.where(md == 0, a[1:2], a[0:1]))

    scale_o, scale_p = pair(scale)
    lse_o, lse_p = pair(lse)
    g_o, g_p = pair(g)
    s_o = scale_o * jnp.exp(origin - lse_o)
    s_p = scale_p * jnp.exp(origin_p - lse_p)
    vecs = jnp.where(row8 == 0, s_o, jnp.where(row8 == 1, g_o, jnp.where(row8 == 2, 2.0 * s_p, jnp.where(row8 == 3, 2.0 * g_p, 0.0))))
    cols_buf[...] = vecs.T

    cross_wait(0)
    cross_wait(1)

    qb = 64

    def quad(i, carry):
        acc_s, acc_g = carry
        rs = columns(i * qb, qb)
        rt = columns(T + i * qb, qb)
        cols = cols_buf[rs, :]
        so, go, sp, gp = (cols[:, k : k + 1] for k in range(4))
        xx = x2[rs, :]
        lhs = so * y[rs, 0:T] + xx * (sp * yx[rs, 0:T] + gp * yx[rt, 0:T])
        rhs = so * y[rs, T : 2 * T] + go * yo[rs, :] + xx * (sp * yx[rs, T : 2 * T] + gp * yx[rt, T : 2 * T])
        acc_s = acc_s + jnp.sum(lhs.reshape(qb // 8, 8, T), axis=0)
        acc_g = acc_g + jnp.sum(rhs.reshape(qb // 8, 8, T), axis=0)
        return acc_s, acc_g

    zero = jnp.zeros((8, T), F32)
    acc_s, acc_g = lax.fori_loop(0, T // qb, quad, (zero, zero))
    q = jnp.sum(jnp.sum(acc_s * s_o + acc_g * g_o, axis=0, keepdims=True), axis=1, keepdims=True)
    fin1[col_id] = jnp.broadcast_to(q, (8, 128))
    share(fin1, col_id, col_peer, 8, fs1, fr1)

    wait_bytes(h2.at[pl.ds(0, T - 8)], hs)
    wait_bytes(x2.at[pl.ds(0, T - 8)], xs)
    wait_bytes(partner_rows, hps)
    wait_bytes(ep, es)
    wait_bytes(ints1.at[pl.ds(0, 7)], is1)
    wait_bytes(ints2.at[pl.ds(0, 15)], is2)
    wait_bytes(st1.reshape(32, 8, 128).at[pl.ds(0, 30)], ss1)
    wait_bytes(st2.at[pl.ds(0, 7)], ss2)
    nll_own, _ = pair(nll)
    turned = pltpu.roll(jnp.broadcast_to(nll_own, (8, T)), (T - item * 8) % T, 1)

    wait_bytes(fin1.at[pl.ds(0, 7)], fr1)
    fin2[plane_id] = sum(fin1[k] for k in range(8))
    share(fin2, plane_id, plane_peer, 16, fs2, fr2)
    wait_bytes(fin1.at[pl.ds(0, 7)], fs1)
    wait_bytes(fin2.at[pl.ds(0, 15)], fr2)
    norm = jnp.sqrt(jnp.maximum(sum(fin2[k] for k in range(16)), 0.0))
    out_ref[...] = jnp.where(
        row8[:, 0:128] == 0, turned[:, 0:128], jnp.where(row8[:, 0:128] == 1, loss, norm[0:1, 0:1]))
    wait_bytes(fin2.at[pl.ds(0, 15)], fs2)


def local(hidden, embedding, targets, mask):
    dma = pltpu.SemaphoreType.DMA
    vmem, smem = pl.BlockSpec(memory_space=pltpu.VMEM), pl.BlockSpec(memory_space=pltpu.SMEM)
    whole = pl.BlockSpec(memory_space=pl.ANY)
    out = pl.pallas_call(
        kernel,
        out_shape=jax.ShapeDtypeStruct((8, 128), F32),
        in_specs=[whole, whole, smem, smem],
        out_specs=vmem,
        scratch_shapes=[
            pltpu.VMEM((T + 8, D), BF16),
            pltpu.VMEM((VOC, D), BF16),
            pltpu.VMEM((VPAD, T), F32),
            pltpu.VMEM((T, T), F32),
            pltpu.VMEM((T, 8), F32),
            pltpu.VMEM((2, 2, 2, 2, 2, 2, 8, T), F32),
            pltpu.VMEM((VPAD, 2 * T), BF16),
            pltpu.VMEM((VPAD // 2, T), BF16),
            pltpu.VMEM((VPAD // 2, T), BF16),
            pltpu.VMEM((T, 2 * T), F32),
            pltpu.VMEM((T, T), F32),
            pltpu.VMEM((2 * T, 2 * T), F32),
            pltpu.VMEM((8, 8, T), jnp.int32),
            pltpu.VMEM((16, 8, T), jnp.int32),
            pltpu.VMEM((2, 16, 8, 128), F32),
            pltpu.VMEM((8, 2, 8, 128), F32),
            pltpu.VMEM((8, 8, 128), F32),
            pltpu.VMEM((16, 8, 128), F32),
            pltpu.VMEM((8, T), F32),
            pltpu.VMEM((8, T), jnp.int32),
            pltpu.VMEM((8, T), F32),
            pltpu.VMEM((T, 8), F32),
            pltpu.VMEM((T, 8), F32),
            dma,
            dma((SLICES,)),
            dma,
            dma((2 * SLICES, 6)),
            dma,
            dma((2, 5)),
            dma, dma, dma, dma((2,)),
            dma, dma, dma, dma,
            dma, dma((2,)), dma, dma,
            dma, dma, dma, dma,
        ],
        compiler_params=pltpu.CompilerParams(collective_id=0, has_side_effects=True),
        name="heads",
    )(hidden, embedding, targets, mask)
    return (out[0:1, 0:8], out[1, 0], out[2, 0])


def solution(mesh):
    torus = Mesh(mesh.devices.reshape(2, 2, 2, 4, 4), ("s", "d", "zl", "y", "x"))
    group = ("s", "zl", "y", "x")
    return jax.shard_map(
        local,
        mesh=torus,
        in_specs=(P("d", group, None), P(group, None), P("d", group), P("d", group)),
        out_specs=(P("d", group), P(), P()),
        check_vma=False,
    )
```

```python
import jax
import jax.numpy as jnp
from jax import lax
from jax.experimental import pallas as pl
from jax.experimental.pallas import tpu as pltpu
from jax.sharding import Mesh
from jax.sharding import PartitionSpec as P

MESH = pl.DeviceIdType.MESH
F32 = jnp.float32
BF16 = jnp.bfloat16

VOC = 1010
VPAD = 1024
D = 7168
T = 512
SLICES = 7
WIDTH = D // SLICES
HALF = T // 2
SUBS = 4
SUBW = WIDTH // SUBS
DIRECT = 7
DOUBLED = 2 * SLICES - DIRECT
LEAD = 2
LAG = 3
SKIP = 3
TURN_R = SKIP + 3 * LAG + 1
TURN_A = TURN_R + SLICES - 1 - DIRECT
NEUTRAL = -1e30
SHIFT = 13.862943611198906
CYCLE = (5, 3, 4, 2)


def kernel(
    hid_ref, emb_ref, tgt_ref, mask_ref, out_ref,
    hx, emb, l, b, xt, xall, w, wp, ep, y, yo, yx,
    ints1, ints2, ints3, st1, st2, fin1, fin2, live_buf, tgt_buf, orig_buf, tcols_buf, cols_buf,
    hid_sem, emb_sem, hs, hr, xs, xr, hps, hpr, es, er,
    is1, ir1, is2, ir2, is3, ir3, ss1, sr1, ss2, sr2, fs1, fr1, fs2, fr2,
):
    ms, md, mz, my, mx = (lax.axis_index(a) for a in ("s", "d", "zl", "y", "x"))
    zz = md * 2 + mz
    qx1, qx0 = mx // 2, (mx + mx // 2) % 2
    qy1, qy0 = my // 2, (my + my // 2) % 2
    mine = (mz, ms, qy1, qy0, qx1, qx0)
    partner = {
        5: {"x": mx + 1 - 2 * (mx % 2)},
        4: {"x": 3 - mx},
        3: {"y": my + 1 - 2 * (my % 2)},
        2: {"y": 3 - my},
    }
    core, other_plane = {"s": 1 - ms}, {"zl": 1 - mz}
    item = ((((mz * 2 + ms) * 2 + qy1) * 2 + qy0) * 2 + qx1) * 2 + qx0
    col_id = ms * 4 + zz
    plane_id = my * 4 + mx
    h2 = hx.at[pl.ds(0, T)]
    h = h2.reshape(2, 2, 2, 2, 2, 2, 8, D)
    partner_rows = hx.at[pl.ds(T, 8)]
    x2 = xall.reshape(T, T)

    def col_peer(k):
        z = (zz + k % 4) % 4
        return {"s": (ms + k // 4) % 2, "d": z // 2, "zl": z % 2}

    def plane_peer(k):
        return {"y": (my + k // 4) % 4, "x": (mx + k % 4) % 4}

    def zx_peer(k):
        return {"zl": (mz + k // 4) % 2, "x": (mx + k % 4) % 4}

    def zy_peer(k):
        return {"zl": (mz + k // 4) % 2, "y": (my + k % 4) % 4}

    def wait_bytes(ref, sem):
        pltpu.make_async_copy(ref, ref, sem).wait()

    def send(src, dst, ssem, rsem, dev):
        pltpu.make_async_remote_copy(
            src_ref=src, dst_ref=dst, send_sem=ssem, recv_sem=rsem,
            device_id=dev, device_id_type=MESH).start()

    own = pltpu.make_async_copy(hid_ref.at[0], h.at[mine], hid_sem)
    own.start()

    def emb_copy(c):
        cs = pl.ds(pl.multiple_of(c * WIDTH, WIDTH), WIDTH)
        return pltpu.make_async_copy(emb_ref.at[:, cs], emb.at[:, cs], emb_sem.at[c])

    barrier = pltpu.get_barrier_semaphore()
    greeted = [col_peer(k) for k in range(1, 8)] + [plane_peer(k) for k in range(1, 16)]
    greeted += [zx_peer(k) for k in range(5, 8)] + [zy_peer(k) for k in range(5, 8)]
    for dev in greeted:
        pl.semaphore_signal(barrier, inc=1, device_id=dev, device_id_type=MESH)
    for c in range(SLICES):
        emb_copy(c).start()

    row8 = lax.broadcasted_iota(jnp.int32, (8, T), 0)
    row16 = lax.broadcasted_iota(jnp.int32, (16, 128), 0)
    lane = lax.broadcasted_iota(jnp.int32, (16, 128), 1)
    ints = jnp.zeros((16, 128), jnp.int32)
    for i in range(8):
        here = lane == (item % 16) * 8 + i
        ints = jnp.where(here & (row16 == md * 4 + item // 16), tgt_ref[0, i], ints)
        ints = jnp.where(here & (row16 == 8 + md * 4 + item // 16), mask_ref[0, i], ints)
    ints1[col_id] = ints
    l[...] = jnp.zeros_like(l)
    b[...] = jnp.zeros_like(b)
    xt[...] = jnp.zeros_like(xt)
    own.wait()
    pl.semaphore_wait(barrier, len(greeted))

    def share(buf, my_slot, peer, count, ssem, rsem):
        for k in range(1, count):
            send(buf.at[my_slot], buf.at[my_slot], ssem, rsem, peer(k))

    def box(held, cs, plane=mz):
        at = (plane, *mine[1:])
        return tuple(slice(None) if dim in held else at[dim] for dim in range(6)) + (slice(None), cs)

    def columns(start, width):
        return pl.ds(pl.multiple_of(start, width), width)

    def slice_wait(unit, stage, items):
        wait_bytes(h2.at[pl.ds(0, 8 * items), pl.ds(0, WIDTH)], hr.at[unit, stage])

    def x_peer(k):
        return {"x": (mx + k) % 4}

    def y_peer(k):
        return {"y": (my + k) % 4}

    def direct_send(c, stage):
        for sub, (first, second, held) in enumerate(((x_peer, y_peer, (4, 5)), (y_peer, x_peer, (2, 3)))):
            cs = columns(c * WIDTH + sub * (WIDTH // 2), WIDTH // 2)
            where = h.at[box(held if stage else (), cs)]
            for k in (2, 1, 3):
                send(where, where, hs, hr.at[c, stage], (second if stage else first)(k))

    def place(unit):
        phase = unit // SLICES
        return unit - phase * SLICES, mz + phase * (1 - 2 * mz), phase

    def cube_send(unit, step):
        c, plane, _ = place(unit)
        for sub in range(SUBS):
            dims = [CYCLE[(sub + k) % 4] for k in range(4)]
            where = h.at[box(dims[:step], columns(c * WIDTH + sub * SUBW, SUBW), plane)]
            send(where, where, hs, hr.at[unit, 1 + step], partner[dims[step]])

    def core_send(unit):
        c, plane, _ = place(unit)
        where = h.at[box((2, 3, 4, 5), columns(c * WIDTH, WIDTH), plane)]
        send(where, where, hs, hr.at[unit, 5], core)

    for c in range(DIRECT):
        direct_send(c, 0)
    for c in range(DIRECT, SLICES):
        cube_send(c, 0)
    send(h.at[mine], partner_rows, hps, hpr, {"d": 1 - md})
    for c in range(SLICES):
        where = h.at[(*mine, slice(None), columns(c * WIDTH, WIDTH))]
        send(where, where, hs, hr.at[SLICES + c, 0], other_plane)
    share(ints1, col_id, col_peer, 8, is1, ir1)

    def nt(lhs, rhs):
        return lax.dot_general(lhs, rhs, (((1,), (1,)), ((), ())), preferred_element_type=F32)

    blk = 128
    groups = blk // 8
    rows = lax.broadcasted_iota(jnp.int32, (blk, HALF), 0)
    half_rows = VPAD // 2
    theirs = pl.ds(pl.multiple_of((1 - md) * half_rows, half_rows), half_rows)
    ours = pl.ds(pl.multiple_of(md * half_rows, half_rows), half_rows)

    def cross_columns(n):
        return tuple(columns(n * HALF + k * (HALF // 2), HALF // 2) for k in range(2))

    def cross_first(n, phase):
        xall[(*mine, slice(None), columns(n * HALF, HALF))] = xt[columns(n * HALF, HALF), :].T
        for k in range(1, 8):
            for sub, (cs, peer) in enumerate(zip(cross_columns(n), (zx_peer, zy_peer))):
                where = xall.at[(*mine, slice(None), cs)]
                send(where, where, xs, xr.at[phase, sub], peer(k))

    def cross_second(phase):
        for sub in range(2):
            wait_bytes(x2.at[pl.ds(0, 56), pl.ds(0, HALF // 2)], xr.at[phase, sub])
        for plane in range(2):
            halves = cross_columns(plane ^ phase)
            for k in (2, 1, 3):
                for sub, (cs, held, peer) in enumerate(zip(halves, ((4, 5), (2, 3)), (y_peer, x_peer))):
                    where = xall.at[box(held, cs, plane)]
                    send(where, where, xs, xr.at[phase, 2 + sub], peer(k))

    def cross_third(phase):
        for sub in range(2):
            wait_bytes(x2.at[pl.ds(0, 192), pl.ds(0, HALF // 2)], xr.at[phase, 2 + sub])
        for plane in range(2):
            where = xall.at[plane, ms, :, :, :, :, :, columns((plane ^ phase) * HALF, HALF)]
            send(where, where, xs, xr.at[phase, 4], core)

    def cross_wait(phase):
        wait_bytes(x2.at[pl.ds(0, 256), pl.ds(0, HALF)], xr.at[phase, 4])

    def finish_half(n, phase):
        ls = columns(n * HALF, HALF)
        cross_first(n, phase)
        own_t = tgt_buf[0:1, ls]

        def peak_body(i, carry):
            peak, chosen = carry
            at = pl.multiple_of(i * blk, blk)
            part = l[pl.ds(at, blk), ls]
            hit = (rows + at) == own_t
            peak = jnp.maximum(peak, jnp.max(part.reshape(groups, 8, HALF), axis=0))
            chosen = chosen + jnp.sum(jnp.where(hit, part, 0.0).reshape(groups, 8, HALF), axis=0)
            return peak, chosen

        peak, chosen = lax.fori_loop(
            0, VPAD // blk, peak_body,
            (jnp.full((8, HALF), NEUTRAL, F32), jnp.zeros((8, HALF), F32)))
        origin = jnp.max(peak, axis=0, keepdims=True) - SHIFT
        chosen = jnp.sum(chosen, axis=0, keepdims=True)

        def exp_body(i, total):
            at = pl.multiple_of(i * blk, blk)
            e = jnp.exp(l[pl.ds(at, blk), ls] - origin)
            hit = (rows + at) == own_t
            w[pl.ds(at, blk), ls] = jnp.where(hit, 0.0, e).astype(BF16)
            w[pl.ds(at, blk), columns(T + n * HALF, HALF)] = jnp.where(hit, 1.0, 0.0).astype(BF16)
            return total + jnp.sum(e.reshape(groups, 8, HALF), axis=0)

        total = lax.fori_loop(0, VPAD // blk, exp_body, jnp.zeros((8, HALF), F32))
        total = jnp.sum(total, axis=0, keepdims=True)
        st1[phase, plane_id] = tile(origin, total, chosen)
        orig_buf[0:1, ls] = origin
        share(st1.at[phase], plane_id, plane_peer, 16, ss1, sr1.at[phase])

    def tile(*lines):
        out = jnp.zeros((8, 128), F32)
        for k, line in enumerate(lines):
            for part in range(2):
                out = jnp.where(row8[:, 0:128] == 2 * k + part, line[:, part * 128 : (part + 1) * 128], out)
        return out

    def merge(parts):
        top = parts[0][0:2]
        for p in parts[1:]:
            top = jnp.maximum(top, p[0:2])
        tot = jnp.zeros((2, 128), F32)
        pick = jnp.zeros((2, 128), F32)
        for p in parts:
            tot = tot + p[2:4] * jnp.exp(p[0:2] - top)
            pick = pick + p[4:6]
        return top, tot, pick

    def plane_merge(n, phase):
        wait_bytes(st1.at[phase, pl.ds(0, 15)], sr1.at[phase])
        top, tot, pick = merge([st1[phase, k] for k in range(16)])
        st2[col_id, n, 0:2] = top
        st2[col_id, n, 2:4] = tot
        st2[col_id, n, 4:6] = pick
        own_origin = orig_buf[0:1, columns(n * HALF, HALF)]
        st2[col_id, n, 6:7] = own_origin[:, 0:128]
        st2[col_id, n, 7:8] = own_origin[:, 128:256]

    def exchange(n, phase):
        ls = columns(n * HALF, HALF)
        send(w.at[theirs, ls], ep.at[:, ls], es, er.at[phase], {"d": 1 - md})

    def body(i, carry):
        @pl.when(i < DIRECT)
        def _():
            slice_wait(i, 0, 3)
            direct_send(i, 1)

        c = i - LEAD

        @pl.when((c >= 0) & (c < DIRECT))
        def _():
            slice_wait(c, 1, 12)
            core_send(c)

        r4 = i - 3 * LAG - SKIP

        @pl.when((r4 >= 0) & (r4 < DOUBLED))
        def _():
            slice_wait(DIRECT + r4, 4, 8)
            core_send(DIRECT + r4)

        for step in (3, 2, 1):
            r = i - (step - 1) * LAG - SKIP

            @pl.when((r >= 0) & (r < DOUBLED))
            def _(r=r, step=step):
                slice_wait(DIRECT + r, step, 2 ** (step - 1))
                cube_send(DIRECT + r, step)

        unit0 = DIRECT + i + LAG - SKIP

        @pl.when((unit0 >= SLICES) & (unit0 < 2 * SLICES))
        def _():
            slice_wait(unit0, 0, 1)
            cube_send(unit0, 0)

        @pl.when(i == 4)
        def _():
            wait_bytes(ints1.at[pl.ds(0, 7)], ir1)
            ints2[mx] = sum(ints1[k] for k in range(8))
            share(ints2, mx, x_peer, 4, is2, ir2)

        @pl.when(i == 7)
        def _():
            wait_bytes(ints2.at[pl.ds(0, 3)], ir2)
            ints3[my] = sum(ints2[k] for k in range(4))
            share(ints3, my, y_peer, 4, is3, ir3)

        @pl.when(i == LEAD + 1)
        def _():
            wait_bytes(partner_rows, hpr)

        @pl.when(((i > LEAD) & (i <= LEAD + DIRECT)) | (i >= TURN_R))
        def _():
            unit = jnp.where(i >= TURN_R, i - TURN_R + DIRECT, i - LEAD - 1)
            c, n, phase = place(unit)
            slice_wait(unit, 5, 16)

            @pl.when(phase == 0)
            def _():
                emb_copy(c).wait()

            cs, ls = columns(c * WIDTH, WIDTH), columns(n * HALF, HALF)
            hn = h2[ls, cs]
            l[0:VOC, ls] += nt(emb[:, cs], hn)
            xt[ls, :] += nt(hn, partner_rows[:, cs])

            @pl.when(phase == 0)
            def _():
                b[ls, ls] += nt(hn, hn)


        @pl.when(i == TURN_A)
        def _():
            wait_bytes(ints3.at[pl.ds(0, 3)], ir3)
            ints = sum(ints3[k] for k in range(4))
            first_id = (ms * 32 + mz * 16 + my * 4 + mx) * VOC
            lines = [
                jnp.concatenate([ints[4 * k + part : 4 * k + part + 1] for part in range(4)], axis=1)
                for k in range(4)
            ]
            local_t = [jnp.where(line - first_id < VOC, line - first_id, -1) for line in lines[:2]]
            tgt_buf[0:1] = jnp.where(md == 0, local_t[0], local_t[1])
            tgt_buf[1:2] = jnp.where(md == 0, local_t[1], local_t[0])
            live_buf[0:1] = lines[2].astype(F32)
            live_buf[1:2] = lines[3].astype(F32)
            tail = l[VOC - 2 : VPAD]
            tail_row = lax.broadcasted_iota(jnp.int32, tail.shape, 0)
            l[VOC - 2 : VPAD] = jnp.where(tail_row < 2, tail, NEUTRAL)
            finish_half(mz, 0)
            exchange(mz, 0)

        @pl.when(i == TURN_A + 2)
        def _():
            other_t = tgt_buf[1:2]
            rows_full = lax.broadcasted_iota(jnp.int32, (blk, T), 0)

            def other_hot(i, carry):
                at = pl.multiple_of(i * blk, blk)
                hit = (rows_full + (at + md * half_rows)) == other_t
                wp[pl.ds(at, blk), :] = jnp.where(hit, 1.0, 0.0).astype(BF16)
                return carry

            lax.fori_loop(0, half_rows // blk, other_hot, 0)

        @pl.when(i == TURN_A + 3)
        def _():
            cross_second(0)

        @pl.when(i == TURN_A + 5)
        def _():
            plane_merge(mz, 0)

        @pl.when(i == TURN_A + 6)
        def _():
            cross_third(0)

        return carry

    lax.fori_loop(0, TURN_R + DOUBLED, body, 0)

    finish_half(1 - mz, 1)
    exchange(1 - mz, 1)

    own_cols, late_cols = columns(mz * HALF, HALF), columns((1 - mz) * HALF, HALF)

    def late_b(c, carry):
        cs = columns(c * (D // 2), D // 2)
        b[:, late_cols] += nt(h2[:, cs], h2[late_cols, cs])
        return carry

    lax.fori_loop(0, 2, late_b, 0)
    b[late_cols, own_cols] = b[own_cols, late_cols].T

    tgt_rows = jnp.where(row8 < 2, jnp.broadcast_to(tgt_buf[0:1], (8, T)), 0).astype(F32)
    tcols_buf[...] = tgt_rows.T

    def tn(lhs, rhs):
        return lax.dot_general(lhs, rhs, (((0,), (0,)), ((), ())), preferred_element_type=F32)

    def gram_own(i, carry):
        rs = columns(i * HALF, HALF)
        lhs = w[:, rs]
        bb = b[rs, :]
        y[rs, 0:T] = tn(lhs, w[:, 0:T]) * bb
        y[rs, T : 2 * T] = tn(lhs, w[:, T : 2 * T]) * (2.0 * bb)
        return carry

    lax.fori_loop(0, 2, gram_own, 0)
    cross_second(1)

    def same_target(i, carry):
        rs = pl.ds(pl.multiple_of(i * 64, 64), 64)
        own_row = tgt_buf[0:1].astype(F32)
        same = (tcols_buf[rs, 0:1] == own_row) & (own_row >= 0.0)
        yo[rs, :] = jnp.where(same, b[rs, :], 0.0)
        return carry

    lax.fori_loop(0, T // 64, same_target, 0)

    plane_merge(1 - mz, 1)
    share(st2, col_id, col_peer, 8, ss2, sr2)

    def gram_hot(i, carry):
        rs = columns(i * HALF, HALF)
        lhs = wp[:, rs]
        for n in range(2):
            yx[columns(T + i * HALF, HALF), n * T : (n + 1) * T] = tn(lhs, w[ours, n * T : (n + 1) * T])
        return carry

    lax.fori_loop(0, 2, gram_hot, 0)

    cross_third(1)

    def gram_cross(half):
        rs = columns(half * HALF, HALF)
        lhs = ep[:, rs]
        for n in range(2):
            yx[rs, n * T : (n + 1) * T] = tn(lhs, w[ours, n * T : (n + 1) * T])

    wait_bytes(ep.at[:, pl.ds(0, HALF)], er.at[0])
    gram_cross(mz)
    wait_bytes(ep.at[:, pl.ds(0, HALF)], er.at[1])
    gram_cross(1 - mz)

    wait_bytes(st2.at[pl.ds(0, 7)], sr2)
    def line(piece):
        return jnp.concatenate([piece(n)[k : k + 1] for n in range(2) for k in range(2)], axis=1)

    def both(first, second):
        return jnp.where(lax.broadcasted_iota(jnp.int32, (2, T), 0) == 0, first, second)

    merged = [[merge([st2[s * 4 + head * 2 + z, n] for s in range(2) for z in range(2)]) for n in range(2)] for head in range(2)]
    top, tot, pick = (both(*(line(lambda n: merged[head][n][k]) for head in range(2))) for k in range(3))
    lse = top + jnp.log(tot)
    nll = lse - pick
    live = live_buf[0:2]
    weight = jnp.where(lax.broadcasted_iota(jnp.int32, (2, 1), 0) == 0, 1.0, 0.3).astype(F32)
    coef = weight / jnp.maximum(jnp.sum(live, axis=1, keepdims=True), 1.0)
    loss = jnp.sum(coef * jnp.sum(live * nll, axis=1, keepdims=True), axis=0, keepdims=True)
    scale = coef * live
    g = (scale * (jnp.exp(pick - lse) - 1.0)).astype(BF16).astype(F32)
    partner_slot = ms * 4 + (1 - md) * 2 + mz
    origin_p = line(lambda n: st2[partner_slot, n, 6:8])
    origin = orig_buf[0:1]

    def pair(a):
        return (jnp.where(md == 0, a[0:1], a[1:2]), jnp.where(md == 0, a[1:2], a[0:1]))

    scale_o, scale_p = pair(scale)
    lse_o, lse_p = pair(lse)
    g_o, g_p = pair(g)
    s_o = scale_o * jnp.exp(origin - lse_o)
    s_p = scale_p * jnp.exp(origin_p - lse_p)
    vecs = jnp.where(row8 == 0, s_o, jnp.where(row8 == 1, g_o, jnp.where(row8 == 2, 2.0 * s_p, jnp.where(row8 == 3, 2.0 * g_p, 0.0))))
    cols_buf[...] = vecs.T

    cross_wait(0)
    cross_wait(1)

    qb = 64

    def quad(i, carry):
        acc_s, acc_g = carry
        rs = columns(i * qb, qb)
        rt = columns(T + i * qb, qb)
        cols = cols_buf[rs, :]
        so, go, sp, gp = (cols[:, k : k + 1] for k in range(4))
        xx = x2[rs, :]
        lhs = so * y[rs, 0:T] + xx * (sp * yx[rs, 0:T] + gp * yx[rt, 0:T])
        rhs = so * y[rs, T : 2 * T] + go * yo[rs, :] + xx * (sp * yx[rs, T : 2 * T] + gp * yx[rt, T : 2 * T])
        acc_s = acc_s + jnp.sum(lhs.reshape(qb // 8, 8, T), axis=0)
        acc_g = acc_g + jnp.sum(rhs.reshape(qb // 8, 8, T), axis=0)
        return acc_s, acc_g

    zero = jnp.zeros((8, T), F32)
    acc_s, acc_g = lax.fori_loop(0, T // qb, quad, (zero, zero))
    q = jnp.sum(jnp.sum(acc_s * s_o + acc_g * g_o, axis=0, keepdims=True), axis=1, keepdims=True)
    fin1[col_id] = jnp.broadcast_to(q, (8, 128))
    share(fin1, col_id, col_peer, 8, fs1, fr1)

    wait_bytes(h2.at[pl.ds(0, T - 8)], hs)
    wait_bytes(x2.at[pl.ds(0, T - 8)], xs)
    wait_bytes(partner_rows, hps)
    wait_bytes(ep, es)
    wait_bytes(ints1.at[pl.ds(0, 7)], is1)
    wait_bytes(ints2.at[pl.ds(0, 3)], is2)
    wait_bytes(ints3.at[pl.ds(0, 3)], is3)
    wait_bytes(st1.reshape(32, 8, 128).at[pl.ds(0, 30)], ss1)
    wait_bytes(st2.at[pl.ds(0, 7)], ss2)
    nll_own, _ = pair(nll)
    turned = pltpu.roll(jnp.broadcast_to(nll_own, (8, T)), (T - item * 8) % T, 1)

    wait_bytes(fin1.at[pl.ds(0, 7)], fr1)
    fin2[plane_id] = sum(fin1[k] for k in range(8))
    share(fin2, plane_id, plane_peer, 16, fs2, fr2)
    wait_bytes(fin1.at[pl.ds(0, 7)], fs1)
    wait_bytes(fin2.at[pl.ds(0, 15)], fr2)
    norm = jnp.sqrt(jnp.maximum(sum(fin2[k] for k in range(16)), 0.0))
    out_ref[...] = jnp.where(
        row8[:, 0:128] == 0, turned[:, 0:128], jnp.where(row8[:, 0:128] == 1, loss, norm[0:1, 0:1]))
    wait_bytes(fin2.at[pl.ds(0, 15)], fs2)


def local(hidden, embedding, targets, mask):
    dma = pltpu.SemaphoreType.DMA
    vmem, smem = pl.BlockSpec(memory_space=pltpu.VMEM), pl.BlockSpec(memory_space=pltpu.SMEM)
    whole = pl.BlockSpec(memory_space=pl.ANY)
    out = pl.pallas_call(
        kernel,
        out_shape=jax.ShapeDtypeStruct((8, 128), F32),
        in_specs=[whole, whole, smem, smem],
        out_specs=vmem,
        scratch_shapes=[
            pltpu.VMEM((T + 8, D), BF16),
            pltpu.VMEM((VOC, D), BF16),
            pltpu.VMEM((VPAD, T), F32),
            pltpu.VMEM((T, T), F32),
            pltpu.VMEM((T, 8), F32),
            pltpu.VMEM((2, 2, 2, 2, 2, 2, 8, T), F32),
            pltpu.VMEM((VPAD, 2 * T), BF16),
            pltpu.VMEM((VPAD // 2, T), BF16),
            pltpu.VMEM((VPAD // 2, T), BF16),
            pltpu.VMEM((T, 2 * T), F32),
            pltpu.VMEM((T, T), F32),
            pltpu.VMEM((2 * T, 2 * T), F32),
            pltpu.VMEM((8, 16, 128), jnp.int32),
            pltpu.VMEM((4, 16, 128), jnp.int32),
            pltpu.VMEM((4, 16, 128), jnp.int32),
            pltpu.VMEM((2, 16, 8, 128), F32),
            pltpu.VMEM((8, 2, 8, 128), F32),
            pltpu.VMEM((8, 8, 128), F32),
            pltpu.VMEM((16, 8, 128), F32),
            pltpu.VMEM((8, T), F32),
            pltpu.VMEM((8, T), jnp.int32),
            pltpu.VMEM((8, T), F32),
            pltpu.VMEM((T, 8), F32),
            pltpu.VMEM((T, 8), F32),
            dma,
            dma((SLICES,)),
            dma,
            dma((2 * SLICES, 6)),
            dma,
            dma((2, 5)),
            dma, dma, dma, dma((2,)),
            dma, dma, dma, dma, dma, dma,
            dma, dma((2,)), dma, dma,
            dma, dma, dma, dma,
        ],
        compiler_params=pltpu.CompilerParams(collective_id=0, has_side_effects=True),
        name="heads",
    )(hidden, embedding, targets, mask)
    return (out[0:1, 0:8], out[1, 0], out[2, 0])


def solution(mesh):
    torus = Mesh(mesh.devices.reshape(2, 2, 2, 4, 4), ("s", "d", "zl", "y", "x"))
    group = ("s", "zl", "y", "x")
    return jax.shard_map(
        local,
        mesh=torus,
        in_specs=(P("d", group, None), P(group, None), P("d", group), P("d", group)),
        out_specs=(P("d", group), P(), P()),
        check_vma=False,
    )
```

```python
import jax
import jax.numpy as jnp
from jax import lax
from jax.experimental import pallas as pl
from jax.experimental.pallas import tpu as pltpu
from jax.sharding import Mesh
from jax.sharding import PartitionSpec as P

MESH = pl.DeviceIdType.MESH
F32 = jnp.float32
BF16 = jnp.bfloat16

VOC = 1010
VPAD = 1024
D = 7168
T = 512
SLICES = 7
WIDTH = D // SLICES
HALF = T // 2
SUBS = 4
SUBW = WIDTH // SUBS
DIRECT = 7
DOUBLED = 2 * SLICES - DIRECT
LEAD = 2
LAG = 3
SKIP = 3
TURN_R = SKIP + 3 * LAG + 1
TURN_A = TURN_R + SLICES - 1 - DIRECT
NEUTRAL = -1e30
SHIFT = 13.862943611198906
CYCLE = (5, 3, 4, 2)


def kernel(
    hid_ref, emb_ref, tgt_ref, mask_ref, out_ref,
    hx, emb, l, b, xt, xall, w, wp, ep, y, yo, yx,
    ints1, ints2, ints3, st1, st2, fin1, fin2, live_buf, tgt_buf, orig_buf, tcols_buf, cols_buf,
    hid_sem, emb_sem, hs, hr, xs, xr, hps, hpr, es, er,
    is1, ir1, is2, ir2, is3, ir3, ss1, sr1, ss2, sr2, fs1, fr1, fs2, fr2,
):
    ms, md, mz, my, mx = (lax.axis_index(a) for a in ("s", "d", "zl", "y", "x"))
    zz = md * 2 + mz
    qx1, qx0 = mx // 2, (mx + mx // 2) % 2
    qy1, qy0 = my // 2, (my + my // 2) % 2
    mine = (mz, ms, qy1, qy0, qx1, qx0)
    partner = {
        5: {"x": mx + 1 - 2 * (mx % 2)},
        4: {"x": 3 - mx},
        3: {"y": my + 1 - 2 * (my % 2)},
        2: {"y": 3 - my},
    }
    core, other_plane = {"s": 1 - ms}, {"zl": 1 - mz}
    item = ((((mz * 2 + ms) * 2 + qy1) * 2 + qy0) * 2 + qx1) * 2 + qx0
    col_id = ms * 4 + zz
    plane_id = my * 4 + mx
    h2 = hx.at[pl.ds(0, T)]
    h = h2.reshape(2, 2, 2, 2, 2, 2, 8, D)
    partner_rows = hx.at[pl.ds(T, 8)]
    x2 = xall.reshape(T, T)

    def col_peer(k):
        z = (zz + k % 4) % 4
        return {"s": (ms + k // 4) % 2, "d": z // 2, "zl": z % 2}

    def plane_peer(k):
        return {"y": (my + k // 4) % 4, "x": (mx + k % 4) % 4}

    def zx_peer(k):
        return {"zl": (mz + k // 4) % 2, "x": (mx + k % 4) % 4}

    def zy_peer(k):
        return {"zl": (mz + k // 4) % 2, "y": (my + k % 4) % 4}

    def wait_bytes(ref, sem):
        pltpu.make_async_copy(ref, ref, sem).wait()

    def send(src, dst, ssem, rsem, dev):
        pltpu.make_async_remote_copy(
            src_ref=src, dst_ref=dst, send_sem=ssem, recv_sem=rsem,
            device_id=dev, device_id_type=MESH).start()

    own = pltpu.make_async_copy(hid_ref.at[0], h.at[mine], hid_sem)
    own.start()

    def emb_copy(c):
        cs = pl.ds(pl.multiple_of(c * WIDTH, WIDTH), WIDTH)
        return pltpu.make_async_copy(emb_ref.at[:, cs], emb.at[:, cs], emb_sem.at[c])

    barrier = pltpu.get_barrier_semaphore()
    greeted = [col_peer(k) for k in range(1, 8)] + [plane_peer(k) for k in range(1, 16)]
    greeted += [zx_peer(k) for k in range(5, 8)] + [zy_peer(k) for k in range(5, 8)]
    for dev in greeted:
        pl.semaphore_signal(barrier, inc=1, device_id=dev, device_id_type=MESH)
    for c in range(SLICES):
        emb_copy(c).start()

    row8 = lax.broadcasted_iota(jnp.int32, (8, T), 0)
    row16 = lax.broadcasted_iota(jnp.int32, (16, 128), 0)
    lane = lax.broadcasted_iota(jnp.int32, (16, 128), 1)
    ints = jnp.zeros((16, 128), jnp.int32)
    for i in range(8):
        here = lane == (item % 16) * 8 + i
        ints = jnp.where(here & (row16 == md * 4 + item // 16), tgt_ref[0, i], ints)
        ints = jnp.where(here & (row16 == 8 + md * 4 + item // 16), mask_ref[0, i], ints)
    ints1[col_id] = ints
    l[...] = jnp.zeros_like(l)
    b[...] = jnp.zeros_like(b)
    xt[...] = jnp.zeros_like(xt)
    own.wait()
    pl.semaphore_wait(barrier, len(greeted))

    def share(buf, my_slot, peer, count, ssem, rsem):
        for k in range(1, count):
            send(buf.at[my_slot], buf.at[my_slot], ssem, rsem, peer(k))

    def box(held, cs, plane=mz):
        at = (plane, *mine[1:])
        return tuple(slice(None) if dim in held else at[dim] for dim in range(6)) + (slice(None), cs)

    def columns(start, width):
        return pl.ds(pl.multiple_of(start, width), width)

    def slice_wait(unit, stage, items):
        wait_bytes(h2.at[pl.ds(0, 8 * items), pl.ds(0, WIDTH)], hr.at[unit, stage])

    def x_peer(k):
        return {"x": (mx + k) % 4}

    def y_peer(k):
        return {"y": (my + k) % 4}

    def direct_send(c, stage):
        for sub, (first, second, held) in enumerate(((x_peer, y_peer, (4, 5)), (y_peer, x_peer, (2, 3)))):
            cs = columns(c * WIDTH + sub * (WIDTH // 2), WIDTH // 2)
            where = h.at[box(held if stage else (), cs)]
            for k in (2, 1, 3):
                send(where, where, hs, hr.at[c, stage], (second if stage else first)(k))

    def place(unit):
        phase = unit // SLICES
        return unit - phase * SLICES, mz + phase * (1 - 2 * mz), phase

    def cube_send(unit, step):
        c, plane, _ = place(unit)
        for sub in range(SUBS):
            dims = [CYCLE[(sub + k) % 4] for k in range(4)]
            where = h.at[box(dims[:step], columns(c * WIDTH + sub * SUBW, SUBW), plane)]
            send(where, where, hs, hr.at[unit, 1 + step], partner[dims[step]])

    def core_send(unit):
        c, plane, _ = place(unit)
        where = h.at[box((2, 3, 4, 5), columns(c * WIDTH, WIDTH), plane)]
        send(where, where, hs, hr.at[unit, 5], core)

    for c in range(DIRECT):
        direct_send(c, 0)
    for c in range(DIRECT, SLICES):
        cube_send(c, 0)
    for c in range(SLICES):
        where = h.at[(*mine, slice(None), columns(c * WIDTH, WIDTH))]
        send(where, where, hs, hr.at[SLICES + c, 0], other_plane)
        if c == 2:
            send(h.at[mine], partner_rows, hps, hpr, {"d": 1 - md})
    share(ints1, col_id, col_peer, 8, is1, ir1)

    def nt(lhs, rhs):
        return lax.dot_general(lhs, rhs, (((1,), (1,)), ((), ())), preferred_element_type=F32)

    blk = 128
    groups = blk // 8
    rows = lax.broadcasted_iota(jnp.int32, (blk, HALF), 0)
    half_rows = VPAD // 2
    theirs = pl.ds(pl.multiple_of((1 - md) * half_rows, half_rows), half_rows)
    ours = pl.ds(pl.multiple_of(md * half_rows, half_rows), half_rows)

    def cross_columns(n):
        return tuple(columns(n * HALF + k * (HALF // 2), HALF // 2) for k in range(2))

    def cross_first(n, phase):
        xall[(*mine, slice(None), columns(n * HALF, HALF))] = xt[columns(n * HALF, HALF), :].T
        for k in range(1, 8):
            for sub, (cs, peer) in enumerate(zip(cross_columns(n), (zx_peer, zy_peer))):
                where = xall.at[(*mine, slice(None), cs)]
                send(where, where, xs, xr.at[phase, sub], peer(k))

    def cross_second(phase):
        for sub in range(2):
            wait_bytes(x2.at[pl.ds(0, 56), pl.ds(0, HALF // 2)], xr.at[phase, sub])
        for plane in range(2):
            halves = cross_columns(plane ^ phase)
            for k in (2, 1, 3):
                for sub, (cs, held, peer) in enumerate(zip(halves, ((4, 5), (2, 3)), (y_peer, x_peer))):
                    where = xall.at[box(held, cs, plane)]
                    send(where, where, xs, xr.at[phase, 2 + sub], peer(k))

    def cross_third(phase):
        for sub in range(2):
            wait_bytes(x2.at[pl.ds(0, 192), pl.ds(0, HALF // 2)], xr.at[phase, 2 + sub])
        for plane in range(2):
            where = xall.at[plane, ms, :, :, :, :, :, columns((plane ^ phase) * HALF, HALF)]
            send(where, where, xs, xr.at[phase, 4], core)

    def cross_wait(phase):
        wait_bytes(x2.at[pl.ds(0, 256), pl.ds(0, HALF)], xr.at[phase, 4])

    def finish_half(n, phase):
        ls = columns(n * HALF, HALF)
        cross_first(n, phase)
        own_t = tgt_buf[0:1, ls]

        def peak_body(i, carry):
            peak, chosen = carry
            at = pl.multiple_of(i * blk, blk)
            part = l[pl.ds(at, blk), ls]
            hit = (rows + at) == own_t
            peak = jnp.maximum(peak, jnp.max(part.reshape(groups, 8, HALF), axis=0))
            chosen = chosen + jnp.sum(jnp.where(hit, part, 0.0).reshape(groups, 8, HALF), axis=0)
            return peak, chosen

        peak, chosen = lax.fori_loop(
            0, VPAD // blk, peak_body,
            (jnp.full((8, HALF), NEUTRAL, F32), jnp.zeros((8, HALF), F32)))
        origin = jnp.max(peak, axis=0, keepdims=True) - SHIFT
        chosen = jnp.sum(chosen, axis=0, keepdims=True)

        def exp_body(i, total):
            at = pl.multiple_of(i * blk, blk)
            e = jnp.exp(l[pl.ds(at, blk), ls] - origin)
            hit = (rows + at) == own_t
            w[pl.ds(at, blk), ls] = jnp.where(hit, 0.0, e).astype(BF16)
            w[pl.ds(at, blk), columns(T + n * HALF, HALF)] = jnp.where(hit, 1.0, 0.0).astype(BF16)
            return total + jnp.sum(e.reshape(groups, 8, HALF), axis=0)

        count = half_rows // blk
        total = lax.fori_loop((1 - md) * count, (2 - md) * count, exp_body, jnp.zeros((8, HALF), F32))
        send(w.at[theirs, ls], ep.at[:, ls], es, er.at[phase], {"d": 1 - md})
        total = lax.fori_loop(md * count, (1 + md) * count, exp_body, total)
        total = jnp.sum(total, axis=0, keepdims=True)
        st1[phase, plane_id] = tile(origin, total, chosen)
        orig_buf[0:1, ls] = origin
        share(st1.at[phase], plane_id, plane_peer, 16, ss1, sr1.at[phase])

    def tile(*lines):
        out = jnp.zeros((8, 128), F32)
        for k, line in enumerate(lines):
            for part in range(2):
                out = jnp.where(row8[:, 0:128] == 2 * k + part, line[:, part * 128 : (part + 1) * 128], out)
        return out

    def merge(parts):
        top = parts[0][0:2]
        for p in parts[1:]:
            top = jnp.maximum(top, p[0:2])
        tot = jnp.zeros((2, 128), F32)
        pick = jnp.zeros((2, 128), F32)
        for p in parts:
            tot = tot + p[2:4] * jnp.exp(p[0:2] - top)
            pick = pick + p[4:6]
        return top, tot, pick

    def plane_merge(n, phase):
        wait_bytes(st1.at[phase, pl.ds(0, 15)], sr1.at[phase])
        top, tot, pick = merge([st1[phase, k] for k in range(16)])
        st2[col_id, n, 0:2] = top
        st2[col_id, n, 2:4] = tot
        st2[col_id, n, 4:6] = pick
        own_origin = orig_buf[0:1, columns(n * HALF, HALF)]
        st2[col_id, n, 6:7] = own_origin[:, 0:128]
        st2[col_id, n, 7:8] = own_origin[:, 128:256]

    def body(i, carry):
        @pl.when(i < DIRECT)
        def _():
            slice_wait(i, 0, 3)
            direct_send(i, 1)

        c = i - LEAD

        @pl.when((c >= 0) & (c < DIRECT))
        def _():
            slice_wait(c, 1, 12)
            core_send(c)

        r4 = i - 3 * LAG - SKIP

        @pl.when((r4 >= 0) & (r4 < DOUBLED))
        def _():
            slice_wait(DIRECT + r4, 4, 8)
            core_send(DIRECT + r4)

        for step in (3, 2, 1):
            r = i - (step - 1) * LAG - SKIP

            @pl.when((r >= 0) & (r < DOUBLED))
            def _(r=r, step=step):
                slice_wait(DIRECT + r, step, 2 ** (step - 1))
                cube_send(DIRECT + r, step)

        unit0 = DIRECT + i + LAG - SKIP

        @pl.when((unit0 >= SLICES) & (unit0 < 2 * SLICES))
        def _():
            slice_wait(unit0, 0, 1)
            cube_send(unit0, 0)

        @pl.when(i == 4)
        def _():
            wait_bytes(ints1.at[pl.ds(0, 7)], ir1)
            ints2[mx] = sum(ints1[k] for k in range(8))
            share(ints2, mx, x_peer, 4, is2, ir2)

        @pl.when(i == 7)
        def _():
            wait_bytes(ints2.at[pl.ds(0, 3)], ir2)
            ints3[my] = sum(ints2[k] for k in range(4))
            share(ints3, my, y_peer, 4, is3, ir3)

        @pl.when(i == LEAD + 1)
        def _():
            wait_bytes(partner_rows, hpr)

        @pl.when(((i > LEAD) & (i <= LEAD + DIRECT)) | (i >= TURN_R))
        def _():
            unit = jnp.where(i >= TURN_R, i - TURN_R + DIRECT, i - LEAD - 1)
            c, n, phase = place(unit)
            slice_wait(unit, 5, 16)

            @pl.when(phase == 0)
            def _():
                emb_copy(c).wait()

            cs, ls = columns(c * WIDTH, WIDTH), columns(n * HALF, HALF)
            hn = h2[ls, cs]
            xt[ls, :] += nt(hn, partner_rows[:, cs])

            @pl.when(phase == 0)
            def _():
                part = nt(jnp.concatenate([hn, emb[:, cs]], axis=0), hn)
                b[ls, ls] += part[:HALF]
                l[0:VOC, ls] += part[HALF:]

            @pl.when(phase == 1)
            def _():
                l[0:VOC, ls] += nt(emb[:, cs], hn)


        @pl.when(i == TURN_A)
        def _():
            wait_bytes(ints3.at[pl.ds(0, 3)], ir3)
            ints = sum(ints3[k] for k in range(4))
            first_id = (ms * 32 + mz * 16 + my * 4 + mx) * VOC
            lines = [
                jnp.concatenate([ints[4 * k + part : 4 * k + part + 1] for part in range(4)], axis=1)
                for k in range(4)
            ]
            local_t = [jnp.where(line - first_id < VOC, line - first_id, -1) for line in lines[:2]]
            tgt_buf[0:1] = jnp.where(md == 0, local_t[0], local_t[1])
            tgt_buf[1:2] = jnp.where(md == 0, local_t[1], local_t[0])
            live_buf[0:1] = lines[2].astype(F32)
            live_buf[1:2] = lines[3].astype(F32)
            tail = l[VOC - 2 : VPAD]
            tail_row = lax.broadcasted_iota(jnp.int32, tail.shape, 0)
            l[VOC - 2 : VPAD] = jnp.where(tail_row < 2, tail, NEUTRAL)
            finish_half(mz, 0)

        @pl.when(i == TURN_A + 2)
        def _():
            other_t = tgt_buf[1:2]
            rows_full = lax.broadcasted_iota(jnp.int32, (blk, T), 0)

            def other_hot(i, carry):
                at = pl.multiple_of(i * blk, blk)
                hit = (rows_full + (at + md * half_rows)) == other_t
                wp[pl.ds(at, blk), :] = jnp.where(hit, 1.0, 0.0).astype(BF16)
                return carry

            lax.fori_loop(0, half_rows // blk, other_hot, 0)

        @pl.when(i == TURN_A + 3)
        def _():
            cross_second(0)

        @pl.when(i == TURN_A + 5)
        def _():
            plane_merge(mz, 0)

        @pl.when(i == TURN_A + 6)
        def _():
            cross_third(0)

        return carry

    lax.fori_loop(0, TURN_R + DOUBLED, body, 0)

    finish_half(1 - mz, 1)

    own_cols, late_cols = columns(mz * HALF, HALF), columns((1 - mz) * HALF, HALF)

    def late_b(c, carry):
        cs = columns(c * (D // 2), D // 2)
        b[:, late_cols] += nt(h2[:, cs], h2[late_cols, cs])
        return carry

    lax.fori_loop(0, 2, late_b, 0)
    b[late_cols, own_cols] = b[own_cols, late_cols].T

    tgt_rows = jnp.where(row8 < 2, jnp.broadcast_to(tgt_buf[0:1], (8, T)), 0).astype(F32)
    tcols_buf[...] = tgt_rows.T

    def tn(lhs, rhs):
        return lax.dot_general(lhs, rhs, (((0,), (0,)), ((), ())), preferred_element_type=F32)

    def gram_own(i, carry):
        rs = columns(i * HALF, HALF)
        lhs = w[:, rs]
        bb = b[rs, :]
        y[rs, 0:T] = tn(lhs, w[:, 0:T]) * bb
        y[rs, T : 2 * T] = tn(lhs, w[:, T : 2 * T]) * (2.0 * bb)
        return carry

    gram_own(mz, 0)
    cross_second(1)
    gram_own(1 - mz, 0)

    def same_target(i, carry):
        rs = pl.ds(pl.multiple_of(i * 64, 64), 64)
        own_row = tgt_buf[0:1].astype(F32)
        same = (tcols_buf[rs, 0:1] == own_row) & (own_row >= 0.0)
        yo[rs, :] = jnp.where(same, b[rs, :], 0.0)
        return carry

    lax.fori_loop(0, T // 64, same_target, 0)

    plane_merge(1 - mz, 1)
    share(st2, col_id, col_peer, 8, ss2, sr2)

    def gram_hot(i, carry):
        rs = columns(i * HALF, HALF)
        lhs = wp[:, rs]
        for n in range(2):
            yx[columns(T + i * HALF, HALF), n * T : (n + 1) * T] = tn(lhs, w[ours, n * T : (n + 1) * T])
        return carry

    lax.fori_loop(0, 2, gram_hot, 0)

    cross_third(1)

    def gram_cross(half):
        rs = columns(half * HALF, HALF)
        lhs = ep[:, rs]
        for n in range(2):
            yx[rs, n * T : (n + 1) * T] = tn(lhs, w[ours, n * T : (n + 1) * T])

    wait_bytes(ep.at[:, pl.ds(0, HALF)], er.at[0])
    gram_cross(mz)
    wait_bytes(ep.at[:, pl.ds(0, HALF)], er.at[1])
    gram_cross(1 - mz)

    wait_bytes(st2.at[pl.ds(0, 7)], sr2)
    def line(piece):
        return jnp.concatenate([piece(n)[k : k + 1] for n in range(2) for k in range(2)], axis=1)

    def both(first, second):
        return jnp.where(lax.broadcasted_iota(jnp.int32, (2, T), 0) == 0, first, second)

    merged = [[merge([st2[s * 4 + head * 2 + z, n] for s in range(2) for z in range(2)]) for n in range(2)] for head in range(2)]
    top, tot, pick = (both(*(line(lambda n: merged[head][n][k]) for head in range(2))) for k in range(3))
    lse = top + jnp.log(tot)
    nll = lse - pick
    live = live_buf[0:2]
    weight = jnp.where(lax.broadcasted_iota(jnp.int32, (2, 1), 0) == 0, 1.0, 0.3).astype(F32)
    coef = weight / jnp.maximum(jnp.sum(live, axis=1, keepdims=True), 1.0)
    loss = jnp.sum(coef * jnp.sum(live * nll, axis=1, keepdims=True), axis=0, keepdims=True)
    scale = coef * live
    g = (scale * (jnp.exp(pick - lse) - 1.0)).astype(BF16).astype(F32)
    partner_slot = ms * 4 + (1 - md) * 2 + mz
    origin_p = line(lambda n: st2[partner_slot, n, 6:8])
    origin = orig_buf[0:1]

    def pair(a):
        return (jnp.where(md == 0, a[0:1], a[1:2]), jnp.where(md == 0, a[1:2], a[0:1]))

    scale_o, scale_p = pair(scale)
    lse_o, lse_p = pair(lse)
    g_o, g_p = pair(g)
    s_o = scale_o * jnp.exp(origin - lse_o)
    s_p = scale_p * jnp.exp(origin_p - lse_p)
    vecs = jnp.where(row8 == 0, s_o, jnp.where(row8 == 1, g_o, jnp.where(row8 == 2, 2.0 * s_p, jnp.where(row8 == 3, 2.0 * g_p, 0.0))))
    cols_buf[...] = vecs.T

    cross_wait(0)
    cross_wait(1)

    qb = 64

    def quad(i, carry):
        acc_s, acc_g = carry
        rs = columns(i * qb, qb)
        rt = columns(T + i * qb, qb)
        cols = cols_buf[rs, :]
        so, go, sp, gp = (cols[:, k : k + 1] for k in range(4))
        xx = x2[rs, :]
        lhs = so * y[rs, 0:T] + xx * (sp * yx[rs, 0:T] + gp * yx[rt, 0:T])
        rhs = so * y[rs, T : 2 * T] + go * yo[rs, :] + xx * (sp * yx[rs, T : 2 * T] + gp * yx[rt, T : 2 * T])
        acc_s = acc_s + jnp.sum(lhs.reshape(qb // 8, 8, T), axis=0)
        acc_g = acc_g + jnp.sum(rhs.reshape(qb // 8, 8, T), axis=0)
        return acc_s, acc_g

    zero = jnp.zeros((8, T), F32)
    acc_s, acc_g = lax.fori_loop(0, T // qb, quad, (zero, zero))
    q = jnp.sum(jnp.sum(acc_s * s_o + acc_g * g_o, axis=0, keepdims=True), axis=1, keepdims=True)
    fin1[col_id] = jnp.broadcast_to(q, (8, 128))
    share(fin1, col_id, col_peer, 8, fs1, fr1)

    wait_bytes(h2.at[pl.ds(0, T - 8)], hs)
    wait_bytes(x2.at[pl.ds(0, T - 8)], xs)
    wait_bytes(partner_rows, hps)
    wait_bytes(ep, es)
    wait_bytes(ints1.at[pl.ds(0, 7)], is1)
    wait_bytes(ints2.at[pl.ds(0, 3)], is2)
    wait_bytes(ints3.at[pl.ds(0, 3)], is3)
    wait_bytes(st1.reshape(32, 8, 128).at[pl.ds(0, 30)], ss1)
    wait_bytes(st2.at[pl.ds(0, 7)], ss2)
    nll_own, _ = pair(nll)
    turned = pltpu.roll(jnp.broadcast_to(nll_own, (8, T)), (T - item * 8) % T, 1)

    wait_bytes(fin1.at[pl.ds(0, 7)], fr1)
    fin2[plane_id] = sum(fin1[k] for k in range(8))
    share(fin2, plane_id, plane_peer, 16, fs2, fr2)
    wait_bytes(fin1.at[pl.ds(0, 7)], fs1)
    wait_bytes(fin2.at[pl.ds(0, 15)], fr2)
    norm = jnp.sqrt(jnp.maximum(sum(fin2[k] for k in range(16)), 0.0))
    out_ref[...] = jnp.where(
        row8[:, 0:128] == 0, turned[:, 0:128], jnp.where(row8[:, 0:128] == 1, loss, norm[0:1, 0:1]))
    wait_bytes(fin2.at[pl.ds(0, 15)], fs2)


def parted(all_ref, nll_ref, loss_ref, norm_ref):
    nll_ref[...] = all_ref[0:1, 0:8]
    loss_ref[...] = all_ref[1:2, 0:1]
    norm_ref[...] = all_ref[2:3, 0:1]


def local(hidden, embedding, targets, mask):
    dma = pltpu.SemaphoreType.DMA
    vmem, smem = pl.BlockSpec(memory_space=pltpu.VMEM), pl.BlockSpec(memory_space=pltpu.SMEM)
    whole = pl.BlockSpec(memory_space=pl.ANY)
    out = pl.pallas_call(
        kernel,
        out_shape=jax.ShapeDtypeStruct((8, 128), F32),
        in_specs=[whole, whole, smem, smem],
        out_specs=vmem,
        scratch_shapes=[
            pltpu.VMEM((T + 8, D), BF16),
            pltpu.VMEM((VOC, D), BF16),
            pltpu.VMEM((VPAD, T), F32),
            pltpu.VMEM((T, T), F32),
            pltpu.VMEM((T, 8), F32),
            pltpu.VMEM((2, 2, 2, 2, 2, 2, 8, T), F32),
            pltpu.VMEM((VPAD, 2 * T), BF16),
            pltpu.VMEM((VPAD // 2, T), BF16),
            pltpu.VMEM((VPAD // 2, T), BF16),
            pltpu.VMEM((T, 2 * T), F32),
            pltpu.VMEM((T, T), F32),
            pltpu.VMEM((2 * T, 2 * T), F32),
            pltpu.VMEM((8, 16, 128), jnp.int32),
            pltpu.VMEM((4, 16, 128), jnp.int32),
            pltpu.VMEM((4, 16, 128), jnp.int32),
            pltpu.VMEM((2, 16, 8, 128), F32),
            pltpu.VMEM((8, 2, 8, 128), F32),
            pltpu.VMEM((8, 8, 128), F32),
            pltpu.VMEM((16, 8, 128), F32),
            pltpu.VMEM((8, T), F32),
            pltpu.VMEM((8, T), jnp.int32),
            pltpu.VMEM((8, T), F32),
            pltpu.VMEM((T, 8), F32),
            pltpu.VMEM((T, 8), F32),
            dma,
            dma((SLICES,)),
            dma,
            dma((2 * SLICES, 6)),
            dma,
            dma((2, 5)),
            dma, dma, dma, dma((2,)),
            dma, dma, dma, dma, dma, dma,
            dma, dma((2,)), dma, dma,
            dma, dma, dma, dma,
        ],
        compiler_params=pltpu.CompilerParams(collective_id=0, has_side_effects=True),
        name="heads",
    )(hidden, embedding, targets, mask)
    one = pl.BlockSpec(memory_space=pltpu.VMEM)
    nll, loss, norm = pl.pallas_call(
        parted,
        out_shape=(jax.ShapeDtypeStruct((1, 8), F32), jax.ShapeDtypeStruct((1, 1), F32), jax.ShapeDtypeStruct((1, 1), F32)),
        in_specs=[one],
        out_specs=(one, one, one),
        name="parted",
    )(out)
    return (nll, loss[0, 0], norm[0, 0])


def solution(mesh):
    torus = Mesh(mesh.devices.reshape(2, 2, 2, 4, 4), ("s", "d", "zl", "y", "x"))
    group = ("s", "zl", "y", "x")
    return jax.shard_map(
        local,
        mesh=torus,
        in_specs=(P("d", group, None), P(group, None), P("d", group), P("d", group)),
        out_specs=(P("d", group), P(), P()),
        check_vma=False,
    )
```

```python
import jax
import jax.numpy as jnp
from jax import lax
from jax.experimental import pallas as pl
from jax.experimental.pallas import tpu as pltpu
from jax.sharding import Mesh
from jax.sharding import PartitionSpec as P

MESH = pl.DeviceIdType.MESH
F32 = jnp.float32
BF16 = jnp.bfloat16

VOC = 1010
VPAD = 1024
D = 7168
T = 512
SLICES = 7
WIDTH = D // SLICES
HALF = T // 2
SUBS = 4
SUBW = WIDTH // SUBS
DIRECT = 7
DOUBLED = 2 * SLICES - DIRECT
LEAD = 3
LAG = 3
SKIP = 3
TURN_R = SKIP + 3 * LAG + 1
TURN_A = TURN_R + SLICES - 1 - DIRECT
NEUTRAL = -1e30
SHIFT = 13.862943611198906
CYCLE = (5, 3, 4, 2)


def kernel(
    hid_ref, emb_ref, tgt_ref, mask_ref, out_ref,
    hx, emb, l, b, xt, xall, w, wp, ep, y, yo, yx,
    ints1, ints2, ints3, st1, st2, fin1, fin2, live_buf, tgt_buf, orig_buf, tcols_buf, cols_buf,
    hid_sem, emb_sem, hs, hr, xs, xr, hps, hpr, es, er,
    is1, ir1, is2, ir2, is3, ir3, ss1, sr1, ss2, sr2, fs1, fr1, fs2, fr2,
):
    ms, md, mz, my, mx = (lax.axis_index(a) for a in ("s", "d", "zl", "y", "x"))
    zz = md * 2 + mz
    qx1, qx0 = mx // 2, (mx + mx // 2) % 2
    qy1, qy0 = my // 2, (my + my // 2) % 2
    mine = (mz, ms, qy1, qy0, qx1, qx0)
    partner = {
        5: {"x": mx + 1 - 2 * (mx % 2)},
        4: {"x": 3 - mx},
        3: {"y": my + 1 - 2 * (my % 2)},
        2: {"y": 3 - my},
    }
    core, other_plane = {"s": 1 - ms}, {"zl": 1 - mz}
    item = ((((mz * 2 + ms) * 2 + qy1) * 2 + qy0) * 2 + qx1) * 2 + qx0
    col_id = ms * 4 + zz
    plane_id = my * 4 + mx
    h2 = hx.at[pl.ds(0, T)]
    h = h2.reshape(2, 2, 2, 2, 2, 2, 8, D)
    partner_rows = hx.at[pl.ds(T, 8)]
    x2 = xall.reshape(T, T)

    def col_peer(k):
        z = (zz + k % 4) % 4
        return {"s": (ms + k // 4) % 2, "d": z // 2, "zl": z % 2}

    def plane_peer(k):
        return {"y": (my + k // 4) % 4, "x": (mx + k % 4) % 4}

    def zx_peer(k):
        return {"zl": (mz + k // 4) % 2, "x": (mx + k % 4) % 4}

    def zy_peer(k):
        return {"zl": (mz + k // 4) % 2, "y": (my + k % 4) % 4}

    def wait_bytes(ref, sem):
        pltpu.make_async_copy(ref, ref, sem).wait()

    def send(src, dst, ssem, rsem, dev):
        pltpu.make_async_remote_copy(
            src_ref=src, dst_ref=dst, send_sem=ssem, recv_sem=rsem,
            device_id=dev, device_id_type=MESH).start()

    own = pltpu.make_async_copy(hid_ref.at[0], h.at[mine], hid_sem)
    own.start()

    def emb_copy(c):
        cs = pl.ds(pl.multiple_of(c * WIDTH, WIDTH), WIDTH)
        return pltpu.make_async_copy(emb_ref.at[:, cs], emb.at[:, cs], emb_sem.at[c])

    barrier = pltpu.get_barrier_semaphore()
    greeted = [col_peer(k) for k in range(1, 8)] + [plane_peer(k) for k in range(1, 16)]
    greeted += [zx_peer(k) for k in range(5, 8)] + [zy_peer(k) for k in range(5, 8)]
    for dev in greeted:
        pl.semaphore_signal(barrier, inc=1, device_id=dev, device_id_type=MESH)
    for c in range(SLICES):
        emb_copy(c).start()

    row8 = lax.broadcasted_iota(jnp.int32, (8, T), 0)
    row16 = lax.broadcasted_iota(jnp.int32, (16, 128), 0)
    lane = lax.broadcasted_iota(jnp.int32, (16, 128), 1)
    ints = jnp.zeros((16, 128), jnp.int32)
    for i in range(8):
        here = lane == (item % 16) * 8 + i
        ints = jnp.where(here & (row16 == md * 4 + item // 16), tgt_ref[0, i], ints)
        ints = jnp.where(here & (row16 == 8 + md * 4 + item // 16), mask_ref[0, i], ints)
    ints1[col_id] = ints
    l[...] = jnp.zeros_like(l)
    b[...] = jnp.zeros_like(b)
    xt[...] = jnp.zeros_like(xt)
    own.wait()
    pl.semaphore_wait(barrier, len(greeted))

    def share(buf, my_slot, peer, count, ssem, rsem):
        for k in range(1, count):
            send(buf.at[my_slot], buf.at[my_slot], ssem, rsem, peer(k))

    def box(held, cs, plane=mz):
        at = (plane, *mine[1:])
        return tuple(slice(None) if dim in held else at[dim] for dim in range(6)) + (slice(None), cs)

    def columns(start, width):
        return pl.ds(pl.multiple_of(start, width), width)

    def slice_wait(unit, stage, items):
        wait_bytes(h2.at[pl.ds(0, 8 * items), pl.ds(0, WIDTH)], hr.at[unit, stage])

    def x_peer(k):
        return {"x": (mx + k) % 4}

    def y_peer(k):
        return {"y": (my + k) % 4}

    def direct_send(c, stage):
        for sub, (first, second, held) in enumerate(((x_peer, y_peer, (4, 5)), (y_peer, x_peer, (2, 3)))):
            cs = columns(c * WIDTH + sub * (WIDTH // 2), WIDTH // 2)
            where = h.at[box(held if stage else (), cs)]
            for k in (2, 1, 3):
                send(where, where, hs, hr.at[c, stage], (second if stage else first)(k))

    def place(unit):
        phase = unit // SLICES
        return unit - phase * SLICES, mz + phase * (1 - 2 * mz), phase

    def cube_send(unit, step):
        c, plane, _ = place(unit)
        for sub in range(SUBS):
            dims = [CYCLE[(sub + k) % 4] for k in range(4)]
            where = h.at[box(dims[:step], columns(c * WIDTH + sub * SUBW, SUBW), plane)]
            send(where, where, hs, hr.at[unit, 1 + step], partner[dims[step]])

    def core_send(unit):
        c, plane, _ = place(unit)
        where = h.at[box((2, 3, 4, 5), columns(c * WIDTH, WIDTH), plane)]
        send(where, where, hs, hr.at[unit, 5], core)

    for c in range(DIRECT):
        direct_send(c, 0)
    for c in range(DIRECT, SLICES):
        cube_send(c, 0)
    for c in range(SLICES):
        where = h.at[(*mine, slice(None), columns(c * WIDTH, WIDTH))]
        send(where, where, hs, hr.at[SLICES + c, 0], other_plane)
        if c == 2:
            send(h.at[mine], partner_rows, hps, hpr, {"d": 1 - md})
    share(ints1, col_id, col_peer, 8, is1, ir1)

    def nt(lhs, rhs):
        return lax.dot_general(lhs, rhs, (((1,), (1,)), ((), ())), preferred_element_type=F32)

    blk = 128
    groups = blk // 8
    rows = lax.broadcasted_iota(jnp.int32, (blk, HALF), 0)
    half_rows = VPAD // 2
    theirs = pl.ds(pl.multiple_of((1 - md) * half_rows, half_rows), half_rows)
    ours = pl.ds(pl.multiple_of(md * half_rows, half_rows), half_rows)

    def cross_columns(n):
        return tuple(columns(n * HALF + k * (HALF // 2), HALF // 2) for k in range(2))

    def cross_first(n, phase):
        xall[(*mine, slice(None), columns(n * HALF, HALF))] = xt[columns(n * HALF, HALF), :].T
        for k in range(1, 8):
            for sub, (cs, peer) in enumerate(zip(cross_columns(n), (zx_peer, zy_peer))):
                where = xall.at[(*mine, slice(None), cs)]
                send(where, where, xs, xr.at[phase, sub], peer(k))

    def cross_second(phase):
        for sub in range(2):
            wait_bytes(x2.at[pl.ds(0, 56), pl.ds(0, HALF // 2)], xr.at[phase, sub])
        for plane in range(2):
            halves = cross_columns(plane ^ phase)
            for k in (2, 1, 3):
                for sub, (cs, held, peer) in enumerate(zip(halves, ((4, 5), (2, 3)), (y_peer, x_peer))):
                    where = xall.at[box(held, cs, plane)]
                    send(where, where, xs, xr.at[phase, 2 + sub], peer(k))

    def cross_third(phase):
        for sub in range(2):
            wait_bytes(x2.at[pl.ds(0, 192), pl.ds(0, HALF // 2)], xr.at[phase, 2 + sub])
        for plane in range(2):
            where = xall.at[plane, ms, :, :, :, :, :, columns((plane ^ phase) * HALF, HALF)]
            send(where, where, xs, xr.at[phase, 4], core)

    def cross_wait(phase):
        wait_bytes(x2.at[pl.ds(0, 256), pl.ds(0, HALF)], xr.at[phase, 4])

    def finish_half(n, phase):
        ls = columns(n * HALF, HALF)
        cross_first(n, phase)
        own_t = tgt_buf[0:1, ls]

        def peak_body(i, carry):
            peak, chosen = carry
            at = pl.multiple_of(i * blk, blk)
            part = l[pl.ds(at, blk), ls]
            hit = (rows + at) == own_t
            peak = jnp.maximum(peak, jnp.max(part.reshape(groups, 8, HALF), axis=0))
            chosen = chosen + jnp.sum(jnp.where(hit, part, 0.0).reshape(groups, 8, HALF), axis=0)
            return peak, chosen

        peak, chosen = lax.fori_loop(
            0, VPAD // blk, peak_body,
            (jnp.full((8, HALF), NEUTRAL, F32), jnp.zeros((8, HALF), F32)))
        origin = jnp.max(peak, axis=0, keepdims=True) - SHIFT
        chosen = jnp.sum(chosen, axis=0, keepdims=True)

        def exp_body(i, total):
            at = pl.multiple_of(i * blk, blk)
            e = jnp.exp(l[pl.ds(at, blk), ls] - origin)
            hit = (rows + at) == own_t
            w[pl.ds(at, blk), ls] = jnp.where(hit, 0.0, e).astype(BF16)
            w[pl.ds(at, blk), columns(T + n * HALF, HALF)] = jnp.where(hit, 1.0, 0.0).astype(BF16)
            return total + jnp.sum(e.reshape(groups, 8, HALF), axis=0)

        count = half_rows // blk
        total = lax.fori_loop((1 - md) * count, (2 - md) * count, exp_body, jnp.zeros((8, HALF), F32))
        send(w.at[theirs, ls], ep.at[:, ls], es, er.at[phase], {"d": 1 - md})
        total = lax.fori_loop(md * count, (1 + md) * count, exp_body, total)
        total = jnp.sum(total, axis=0, keepdims=True)
        st1[phase, plane_id] = tile(origin, total, chosen)
        orig_buf[0:1, ls] = origin
        share(st1.at[phase], plane_id, plane_peer, 16, ss1, sr1.at[phase])

    def tile(*lines):
        out = jnp.zeros((8, 128), F32)
        for k, line in enumerate(lines):
            for part in range(2):
                out = jnp.where(row8[:, 0:128] == 2 * k + part, line[:, part * 128 : (part + 1) * 128], out)
        return out

    def merge(parts):
        top = parts[0][0:2]
        for p in parts[1:]:
            top = jnp.maximum(top, p[0:2])
        tot = jnp.zeros((2, 128), F32)
        pick = jnp.zeros((2, 128), F32)
        for p in parts:
            tot = tot + p[2:4] * jnp.exp(p[0:2] - top)
            pick = pick + p[4:6]
        return top, tot, pick

    def plane_merge(n, phase):
        wait_bytes(st1.at[phase, pl.ds(0, 15)], sr1.at[phase])
        top, tot, pick = merge([st1[phase, k] for k in range(16)])
        st2[col_id, n, 0:2] = top
        st2[col_id, n, 2:4] = tot
        st2[col_id, n, 4:6] = pick
        own_origin = orig_buf[0:1, columns(n * HALF, HALF)]
        st2[col_id, n, 6:7] = own_origin[:, 0:128]
        st2[col_id, n, 7:8] = own_origin[:, 128:256]

    def body(i, carry):
        @pl.when(i < DIRECT)
        def _():
            slice_wait(i, 0, 3)
            direct_send(i, 1)

        c = i - LEAD

        @pl.when((c >= 0) & (c < DIRECT))
        def _():
            slice_wait(c, 1, 12)
            core_send(c)

        r4 = i - 3 * LAG - SKIP

        @pl.when((r4 >= 0) & (r4 < DOUBLED))
        def _():
            slice_wait(DIRECT + r4, 4, 8)
            core_send(DIRECT + r4)

        for step in (3, 2, 1):
            r = i - (step - 1) * LAG - SKIP

            @pl.when((r >= 0) & (r < DOUBLED))
            def _(r=r, step=step):
                slice_wait(DIRECT + r, step, 2 ** (step - 1))
                cube_send(DIRECT + r, step)

        unit0 = DIRECT + i + LAG - SKIP

        @pl.when((unit0 >= SLICES) & (unit0 < 2 * SLICES))
        def _():
            slice_wait(unit0, 0, 1)
            cube_send(unit0, 0)

        @pl.when(i == 4)
        def _():
            wait_bytes(ints1.at[pl.ds(0, 7)], ir1)
            ints2[mx] = sum(ints1[k] for k in range(8))
            share(ints2, mx, x_peer, 4, is2, ir2)

        @pl.when(i == 7)
        def _():
            wait_bytes(ints2.at[pl.ds(0, 3)], ir2)
            ints3[my] = sum(ints2[k] for k in range(4))
            share(ints3, my, y_peer, 4, is3, ir3)

        @pl.when(i == LEAD + 1)
        def _():
            wait_bytes(partner_rows, hpr)

        @pl.when(((i > LEAD) & (i <= LEAD + DIRECT)) | (i >= TURN_R))
        def _():
            unit = jnp.where(i >= TURN_R, i - TURN_R + DIRECT, i - LEAD - 1)
            c, n, phase = place(unit)
            slice_wait(unit, 5, 16)

            @pl.when(phase == 0)
            def _():
                emb_copy(c).wait()

            cs, ls = columns(c * WIDTH, WIDTH), columns(n * HALF, HALF)
            hn = h2[ls, cs]

            @pl.when(phase == 0)
            def _():
                xt[ls, :] += nt(hn, partner_rows[:, cs])
                part = nt(jnp.concatenate([hn, emb[:, cs]], axis=0), hn)
                b[ls, ls] += part[:HALF]
                l[0:VOC, ls] += part[HALF:]

            @pl.when(phase == 1)
            def _():
                l[0:VOC, ls] += nt(emb[:, cs], hn)
                xt[ls, :] += nt(hn, partner_rows[:, cs])


        @pl.when(i == TURN_A)
        def _():
            wait_bytes(ints3.at[pl.ds(0, 3)], ir3)
            ints = sum(ints3[k] for k in range(4))
            first_id = (ms * 32 + mz * 16 + my * 4 + mx) * VOC
            lines = [
                jnp.concatenate([ints[4 * k + part : 4 * k + part + 1] for part in range(4)], axis=1)
                for k in range(4)
            ]
            local_t = [jnp.where(line - first_id < VOC, line - first_id, -1) for line in lines[:2]]
            tgt_buf[0:1] = jnp.where(md == 0, local_t[0], local_t[1])
            tgt_buf[1:2] = jnp.where(md == 0, local_t[1], local_t[0])
            live_buf[0:1] = lines[2].astype(F32)
            live_buf[1:2] = lines[3].astype(F32)
            tail = l[VOC - 2 : VPAD]
            tail_row = lax.broadcasted_iota(jnp.int32, tail.shape, 0)
            l[VOC - 2 : VPAD] = jnp.where(tail_row < 2, tail, NEUTRAL)
            finish_half(mz, 0)

        @pl.when(i == TURN_A + 2)
        def _():
            other_t = tgt_buf[1:2]
            rows_full = lax.broadcasted_iota(jnp.int32, (blk, T), 0)

            def other_hot(i, carry):
                at = pl.multiple_of(i * blk, blk)
                hit = (rows_full + (at + md * half_rows)) == other_t
                wp[pl.ds(at, blk), :] = jnp.where(hit, 1.0, 0.0).astype(BF16)
                return carry

            lax.fori_loop(0, half_rows // blk, other_hot, 0)

        @pl.when(i == TURN_A + 3)
        def _():
            cross_second(0)

        @pl.when(i == TURN_A + 5)
        def _():
            plane_merge(mz, 0)

        @pl.when(i == TURN_A + 6)
        def _():
            cross_third(0)

        return carry

    lax.fori_loop(0, TURN_R + DOUBLED, body, 0)

    finish_half(1 - mz, 1)

    own_cols, late_cols = columns(mz * HALF, HALF), columns((1 - mz) * HALF, HALF)

    def late_b(c, carry):
        cs = columns(c * (D // 2), D // 2)
        b[:, late_cols] += nt(h2[:, cs], h2[late_cols, cs])
        return carry

    lax.fori_loop(0, 2, late_b, 0)
    b[late_cols, own_cols] = b[own_cols, late_cols].T

    tgt_rows = jnp.where(row8 < 2, jnp.broadcast_to(tgt_buf[0:1], (8, T)), 0).astype(F32)
    tcols_buf[...] = tgt_rows.T

    def tn(lhs, rhs):
        return lax.dot_general(lhs, rhs, (((0,), (0,)), ((), ())), preferred_element_type=F32)

    def gram_own(i, carry):
        rs = columns(i * HALF, HALF)
        lhs = w[:, rs]
        bb = b[rs, :]
        y[rs, 0:T] = tn(lhs, w[:, 0:T]) * bb
        y[rs, T : 2 * T] = tn(lhs, w[:, T : 2 * T]) * (2.0 * bb)
        return carry

    gram_own(mz, 0)
    cross_second(1)
    gram_own(1 - mz, 0)

    def same_target(i, carry):
        rs = pl.ds(pl.multiple_of(i * 64, 64), 64)
        own_row = tgt_buf[0:1].astype(F32)
        same = (tcols_buf[rs, 0:1] == own_row) & (own_row >= 0.0)
        yo[rs, :] = jnp.where(same, b[rs, :], 0.0)
        return carry

    lax.fori_loop(0, T // 64, same_target, 0)

    plane_merge(1 - mz, 1)
    share(st2, col_id, col_peer, 8, ss2, sr2)

    def gram_hot(i, carry):
        rs = columns(i * HALF, HALF)
        lhs = wp[:, rs]
        for n in range(2):
            yx[columns(T + i * HALF, HALF), n * T : (n + 1) * T] = tn(lhs, w[ours, n * T : (n + 1) * T])
        return carry

    lax.fori_loop(0, 2, gram_hot, 0)

    cross_third(1)

    def gram_cross(half):
        rs = columns(half * HALF, HALF)
        lhs = ep[:, rs]
        for n in range(2):
            yx[rs, n * T : (n + 1) * T] = tn(lhs, w[ours, n * T : (n + 1) * T])

    wait_bytes(ep.at[:, pl.ds(0, HALF)], er.at[0])
    gram_cross(mz)
    wait_bytes(ep.at[:, pl.ds(0, HALF)], er.at[1])
    gram_cross(1 - mz)

    wait_bytes(st2.at[pl.ds(0, 7)], sr2)
    def line(piece):
        return jnp.concatenate([piece(n)[k : k + 1] for n in range(2) for k in range(2)], axis=1)

    def both(first, second):
        return jnp.where(lax.broadcasted_iota(jnp.int32, (2, T), 0) == 0, first, second)

    merged = [[merge([st2[s * 4 + head * 2 + z, n] for s in range(2) for z in range(2)]) for n in range(2)] for head in range(2)]
    top, tot, pick = (both(*(line(lambda n: merged[head][n][k]) for head in range(2))) for k in range(3))
    lse = top + jnp.log(tot)
    nll = lse - pick
    live = live_buf[0:2]
    weight = jnp.where(lax.broadcasted_iota(jnp.int32, (2, 1), 0) == 0, 1.0, 0.3).astype(F32)
    coef = weight / jnp.maximum(jnp.sum(live, axis=1, keepdims=True), 1.0)
    loss = jnp.sum(coef * jnp.sum(live * nll, axis=1, keepdims=True), axis=0, keepdims=True)
    scale = coef * live
    g = (scale * (jnp.exp(pick - lse) - 1.0)).astype(BF16).astype(F32)
    partner_slot = ms * 4 + (1 - md) * 2 + mz
    origin_p = line(lambda n: st2[partner_slot, n, 6:8])
    origin = orig_buf[0:1]

    def pair(a):
        return (jnp.where(md == 0, a[0:1], a[1:2]), jnp.where(md == 0, a[1:2], a[0:1]))

    scale_o, scale_p = pair(scale)
    lse_o, lse_p = pair(lse)
    g_o, g_p = pair(g)
    s_o = scale_o * jnp.exp(origin - lse_o)
    s_p = scale_p * jnp.exp(origin_p - lse_p)
    vecs = jnp.where(row8 == 0, s_o, jnp.where(row8 == 1, g_o, jnp.where(row8 == 2, 2.0 * s_p, jnp.where(row8 == 3, 2.0 * g_p, 0.0))))
    cols_buf[...] = vecs.T

    cross_wait(0)
    cross_wait(1)

    qb = 64

    def quad(i, carry):
        acc_s, acc_g = carry
        rs = columns(i * qb, qb)
        rt = columns(T + i * qb, qb)
        cols = cols_buf[rs, :]
        so, go, sp, gp = (cols[:, k : k + 1] for k in range(4))
        xx = x2[rs, :]
        lhs = so * y[rs, 0:T] + xx * (sp * yx[rs, 0:T] + gp * yx[rt, 0:T])
        rhs = so * y[rs, T : 2 * T] + go * yo[rs, :] + xx * (sp * yx[rs, T : 2 * T] + gp * yx[rt, T : 2 * T])
        acc_s = acc_s + jnp.sum(lhs.reshape(qb // 8, 8, T), axis=0)
        acc_g = acc_g + jnp.sum(rhs.reshape(qb // 8, 8, T), axis=0)
        return acc_s, acc_g

    zero = jnp.zeros((8, T), F32)
    acc_s, acc_g = lax.fori_loop(0, T // qb, quad, (zero, zero))
    q = jnp.sum(jnp.sum(acc_s * s_o + acc_g * g_o, axis=0, keepdims=True), axis=1, keepdims=True)
    fin1[col_id] = jnp.broadcast_to(q, (8, 128))
    share(fin1, col_id, col_peer, 8, fs1, fr1)

    wait_bytes(h2.at[pl.ds(0, T - 8)], hs)
    wait_bytes(x2.at[pl.ds(0, T - 8)], xs)
    wait_bytes(partner_rows, hps)
    wait_bytes(ep, es)
    wait_bytes(ints1.at[pl.ds(0, 7)], is1)
    wait_bytes(ints2.at[pl.ds(0, 3)], is2)
    wait_bytes(ints3.at[pl.ds(0, 3)], is3)
    wait_bytes(st1.reshape(32, 8, 128).at[pl.ds(0, 30)], ss1)
    wait_bytes(st2.at[pl.ds(0, 7)], ss2)
    nll_own, _ = pair(nll)
    turned = pltpu.roll(jnp.broadcast_to(nll_own, (8, T)), (T - item * 8) % T, 1)

    wait_bytes(fin1.at[pl.ds(0, 7)], fr1)
    fin2[plane_id] = sum(fin1[k] for k in range(8))
    share(fin2, plane_id, plane_peer, 16, fs2, fr2)
    wait_bytes(fin1.at[pl.ds(0, 7)], fs1)
    wait_bytes(fin2.at[pl.ds(0, 15)], fr2)
    norm = jnp.sqrt(jnp.maximum(sum(fin2[k] for k in range(16)), 0.0))
    out_ref[...] = jnp.where(
        row8[:, 0:128] == 0, turned[:, 0:128], jnp.where(row8[:, 0:128] == 1, loss, norm[0:1, 0:1]))
    wait_bytes(fin2.at[pl.ds(0, 15)], fs2)


def parted(all_ref, nll_ref, loss_ref, norm_ref):
    nll_ref[...] = all_ref[0:1, 0:8]
    loss_ref[...] = all_ref[1:2, 0:1]
    norm_ref[...] = all_ref[2:3, 0:1]


def local(hidden, embedding, targets, mask):
    dma = pltpu.SemaphoreType.DMA
    vmem, smem = pl.BlockSpec(memory_space=pltpu.VMEM), pl.BlockSpec(memory_space=pltpu.SMEM)
    whole = pl.BlockSpec(memory_space=pl.ANY)
    out = pl.pallas_call(
        kernel,
        out_shape=jax.ShapeDtypeStruct((8, 128), F32),
        in_specs=[whole, whole, smem, smem],
        out_specs=vmem,
        scratch_shapes=[
            pltpu.VMEM((T + 8, D), BF16),
            pltpu.VMEM((VOC, D), BF16),
            pltpu.VMEM((VPAD, T), F32),
            pltpu.VMEM((T, T), F32),
            pltpu.VMEM((T, 8), F32),
            pltpu.VMEM((2, 2, 2, 2, 2, 2, 8, T), F32),
            pltpu.VMEM((VPAD, 2 * T), BF16),
            pltpu.VMEM((VPAD // 2, T), BF16),
            pltpu.VMEM((VPAD // 2, T), BF16),
            pltpu.VMEM((T, 2 * T), F32),
            pltpu.VMEM((T, T), F32),
            pltpu.VMEM((2 * T, 2 * T), F32),
            pltpu.VMEM((8, 16, 128), jnp.int32),
            pltpu.VMEM((4, 16, 128), jnp.int32),
            pltpu.VMEM((4, 16, 128), jnp.int32),
            pltpu.VMEM((2, 16, 8, 128), F32),
            pltpu.VMEM((8, 2, 8, 128), F32),
            pltpu.VMEM((8, 8, 128), F32),
            pltpu.VMEM((16, 8, 128), F32),
            pltpu.VMEM((8, T), F32),
            pltpu.VMEM((8, T), jnp.int32),
            pltpu.VMEM((8, T), F32),
            pltpu.VMEM((T, 8), F32),
            pltpu.VMEM((T, 8), F32),
            dma,
            dma((SLICES,)),
            dma,
            dma((2 * SLICES, 6)),
            dma,
            dma((2, 5)),
            dma, dma, dma, dma((2,)),
            dma, dma, dma, dma, dma, dma,
            dma, dma((2,)), dma, dma,
            dma, dma, dma, dma,
        ],
        compiler_params=pltpu.CompilerParams(collective_id=0, has_side_effects=True),
        name="heads",
    )(hidden, embedding, targets, mask)
    one = pl.BlockSpec(memory_space=pltpu.VMEM)
    nll, loss, norm = pl.pallas_call(
        parted,
        out_shape=(jax.ShapeDtypeStruct((1, 8), F32), jax.ShapeDtypeStruct((1, 1), F32), jax.ShapeDtypeStruct((1, 1), F32)),
        in_specs=[one],
        out_specs=(one, one, one),
        name="parted",
    )(out)
    return (nll, loss[0, 0], norm[0, 0])


def solution(mesh):
    torus = Mesh(mesh.devices.reshape(2, 2, 2, 4, 4), ("s", "d", "zl", "y", "x"))
    group = ("s", "zl", "y", "x")
    return jax.shard_map(
        local,
        mesh=torus,
        in_specs=(P("d", group, None), P(group, None), P("d", group), P("d", group)),
        out_specs=(P("d", group), P(), P()),
        check_vma=False,
    )
```
